16 devices in a mesh: data: 2 (over z), expert: 8 (over y, x, core).
Axes of the slice: x: 2, y: 2, z: 2, core: 2. Of those that a mesh axis runs over, the one named last changes fastest.
Arguments:
- dy: bfloat16 [32768, 768], P(('data', 'expert'))
- gates: float32 [32768, 1], P(('data', 'expert'))
- topk_idx: int32 [32768, 1], P(('data', 'expert'))
- slot: int32 [32768, 1], P(('data', 'expert'))
- yd: bfloat16 [32768, 1, 768], P(('data', 'expert'))
- xd: bfloat16 [16, 2560, 768], P(('data', 'expert'))
- h1: bfloat16 [16, 2560, 3072], P(('data', 'expert'))
- h3: bfloat16 [16, 2560, 3072], P(('data', 'expert'))
- w1: bfloat16 [8, 768, 3072], P('expert')
- w3: bfloat16 [8, 768, 3072], P('expert')
- w2: bfloat16 [8, 3072, 768], P('expert')
Outputs:
- output 1: bfloat16 [32768, 768], P(('data', 'expert'))
- output 2: float32 [32768, 1], P(('data', 'expert'))
- output 3: float32 [8, 768, 3072], P('expert', None, 'data')
- output 4: float32 [8, 768, 3072], P('expert', None, 'data')
- output 5: float32 [8, 3072, 768], P('expert', 'data')
All inputs are finite; a program needn't handle non-finite values.
Results may differ from the reference program's by a relative error of at most 0.0106822.
Values are sent between devices in bfloat16 or wider.
A program may use at most 1 GiB of HBM per device.

```python
import jax
import jax.numpy as jnp
from jax import lax

NDATA = 2
NEXP = 8
TOKENS = 2048
EXPERTS = 8
TOPK = 1
DMODEL = 768
FF = 3072
CAP = 320

NTOK = NDATA * NEXP * TOKENS
NDEV = NDATA * NEXP
NBUF = NEXP * CAP


def _routes(topk_idx, slot):
    dev = jnp.arange(NTOK, dtype=jnp.int32) // TOKENS
    row = (dev // NEXP)[:, None] * EXPERTS + topk_idx
    col = jnp.where(slot >= 0, (dev % NEXP)[:, None] * CAP + slot, NBUF)
    return row, col


def _slots(topk_idx):
    def one(idx):
        oh = (idx.reshape(-1)[:, None] == jnp.arange(EXPERTS, dtype=jnp.int32)[None, :]).astype(jnp.int32)
        rank = jnp.sum((jnp.cumsum(oh, axis=0) - oh) * oh, axis=1)
        return jnp.where(rank < CAP, rank, -1).reshape(TOKENS, TOPK)
    return lax.map(one, topk_idx.reshape(NDEV, TOKENS, TOPK)).reshape(NTOK, TOPK).astype(jnp.int32)


def _forward(x, topk_idx, slot, w1, w3, w2):
    row, col = _routes(topk_idx, slot)
    xin = jnp.broadcast_to(x[:, None, :], (NTOK, TOPK, DMODEL))
    xd = jnp.zeros((NDATA * EXPERTS, NBUF, DMODEL), jnp.bfloat16).at[row, col].set(xin, mode='drop')
    x4 = xd.reshape(NDATA, EXPERTS, NBUF, DMODEL)

    def one(e):
        xs = x4[:, e].reshape(NDATA * NBUF, DMODEL)
        h1 = jnp.dot(xs, w1[e], preferred_element_type=jnp.float32).astype(jnp.bfloat16)
        h3 = jnp.dot(xs, w3[e], preferred_element_type=jnp.float32).astype(jnp.bfloat16)
        h1f = h1.astype(jnp.float32)
        a = (h1f * jax.nn.sigmoid(h1f) * h3.astype(jnp.float32)).astype(jnp.bfloat16)
        y = jnp.dot(a, w2[e], preferred_element_type=jnp.float32).astype(jnp.bfloat16)
        return h1.reshape(NDATA, NBUF, FF), h3.reshape(NDATA, NBUF, FF), y.reshape(NDATA, NBUF, DMODEL)

    h1, h3, y = lax.map(one, jnp.arange(EXPERTS))
    flat = lambda a: jnp.swapaxes(a, 0, 1).reshape(NDATA * EXPERTS, NBUF, a.shape[-1])
    h1, h3, y = flat(h1), flat(h3), flat(y)
    yd = jnp.where((slot >= 0)[:, :, None], y[row, jnp.minimum(col, NBUF - 1)], jnp.zeros((), jnp.bfloat16))
    return xd, h1, h3, yd


def _draw_routes(bias_key, pick_key):
    level_parts = jax.random.randint(bias_key, (4, NDEV, EXPERTS), 0, 4, jnp.int32)
    levels = jnp.sum(level_parts, axis=0)
    weights = jnp.left_shift(jnp.ones_like(levels), levels)
    tok_dev = jnp.arange(NTOK, dtype=jnp.int32) // TOKENS
    row_weights = weights[tok_dev]
    pick_keys = jax.random.split(pick_key, TOPK)
    columns = jnp.arange(EXPERTS, dtype=jnp.int32)[None, :]
    chosen = []
    for choice_idx in range(TOPK):
        bounds = jnp.cumsum(row_weights, axis=1)
        draw_value = jax.random.randint(pick_keys[choice_idx], (NTOK,), 0, bounds[:, -1], jnp.int32)
        pick_now = jnp.sum(bounds <= draw_value[:, None], axis=1, dtype=jnp.int32)
        chosen.append(pick_now)
        row_weights = jnp.where(columns == pick_now[:, None], 0, row_weights)
    return jnp.stack(chosen, axis=1).astype(jnp.int32)


def setup_inputs(seed: int = 0) -> dict:
    ks = jax.random.split(jax.random.PRNGKey(seed), 8)
    x = jax.random.normal(ks[0], (NTOK, DMODEL), jnp.float32).astype(jnp.bfloat16)
    w1 = (jax.random.normal(ks[1], (EXPERTS, DMODEL, FF), jnp.float32) * DMODEL ** -0.5).astype(jnp.bfloat16)
    w3 = (jax.random.normal(ks[2], (EXPERTS, DMODEL, FF), jnp.float32) * DMODEL ** -0.5).astype(jnp.bfloat16)
    w2 = (jax.random.normal(ks[3], (EXPERTS, FF, DMODEL), jnp.float32) * FF ** -0.5).astype(jnp.bfloat16)
    rk = jax.random.split(jax.random.fold_in(ks[4], 7), 2)
    topk_idx = _draw_routes(rk[0], rk[1])
    slot = _slots(topk_idx)
    gates = jax.random.uniform(ks[5], (NTOK, TOPK), jnp.float32, 0.2, 1.0)
    dy = jax.random.normal(ks[6], (NTOK, DMODEL), jnp.float32).astype(jnp.bfloat16)
    xd, h1, h3, yd = _forward(x, topk_idx, slot, w1, w3, w2)
    return dict(dy=dy, gates=gates, topk_idx=topk_idx, slot=slot, yd=yd, xd=xd, h1=h1, h3=h3, w1=w1, w3=w3, w2=w2)


def reference(dy, gates, topk_idx, slot, yd, xd, h1, h3, w1, w3, w2):
    row, col = _routes(topk_idx, slot)
    dyf = dy.astype(jnp.float32)
    dg = jnp.sum(yd.astype(jnp.float32) * dyf[:, None, :], axis=-1)
    v = (gates[:, :, None] * dyf[:, None, :]).astype(jnp.bfloat16)
    dyd = jnp.zeros((NDATA * EXPERTS, NBUF, DMODEL), jnp.bfloat16).at[row, col].set(v, mode='drop')
    grp = lambda a: a.reshape(NDATA, EXPERTS, NBUF, a.shape[-1])
    g4, x4, a14, a34 = grp(dyd), grp(xd), grp(h1), grp(h3)

    def one(e):
        g = g4[:, e].reshape(NDATA * NBUF, DMODEL)
        x = x4[:, e].reshape(NDATA * NBUF, DMODEL)
        h1f = a14[:, e].reshape(NDATA * NBUF, FF).astype(jnp.float32)
        h3f = a34[:, e].reshape(NDATA * NBUF, FF).astype(jnp.float32)
        s = jax.nn.sigmoid(h1f)
        silu = h1f * s
        a = (silu * h3f).astype(jnp.bfloat16)
        da = jnp.dot(g, w2[e].T, preferred_element_type=jnp.float32).astype(jnp.bfloat16).astype(jnp.float32)
        dh1 = (da * h3f * s * (1.0 + h1f * (1.0 - s))).astype(jnp.bfloat16)
        dh3 = (da * silu).astype(jnp.bfloat16)
        dw2 = jnp.dot(a.T, g, preferred_element_type=jnp.float32)
        dw1 = jnp.dot(x.T, dh1, preferred_element_type=jnp.float32)
        dw3 = jnp.dot(x.T, dh3, preferred_element_type=jnp.float32)
        dxd = (jnp.dot(dh1, w1[e].T, preferred_element_type=jnp.float32)
               + jnp.dot(dh3, w3[e].T, preferred_element_type=jnp.float32)).astype(jnp.bfloat16)
        return dw1, dw3, dw2, dxd.reshape(NDATA, NBUF, DMODEL)

    dw1, dw3, dw2, dxd = lax.map(one, jnp.arange(EXPERTS))
    dxd = jnp.swapaxes(dxd, 0, 1).reshape(NDATA * EXPERTS, NBUF, DMODEL)
    back = dxd[row, jnp.minimum(col, NBUF - 1)].astype(jnp.float32)
    dx = jnp.sum(jnp.where((slot >= 0)[:, :, None], back, 0.0), axis=1).astype(jnp.bfloat16)
    return dx, dg, dw1, dw3, dw2
```

```python
import functools

import jax
import jax.numpy as jnp
from jax import lax
from jax.experimental import pallas as pl
from jax.experimental.pallas import tpu as pltpu
from jax.sharding import PartitionSpec as P

F32 = jnp.float32
BF16 = jnp.bfloat16
I32 = jnp.int32


TILE = 64
BT = 8
FC = 768
VMEM_LIMIT = 62 * 1024 * 1024

ANY = pl.BlockSpec(memory_space=pl.ANY)
HBM = pl.BlockSpec(memory_space=pltpu.HBM)
SMEM = pl.BlockSpec(memory_space=pltpu.SMEM)


def _params(**kw):
    return pltpu.CompilerParams(vmem_limit_bytes=VMEM_LIMIT, **kw)


def _cost(flops, nbytes):
    return pl.CostEstimate(flops=int(flops), bytes_accessed=int(nbytes), transcendentals=0)


def _dot(a, b):
    return jnp.dot(a, b, preferred_element_type=F32)


def _dot_tn(a, b):
    return lax.dot_general(a, b, (((0,), (0,)), ((), ())), preferred_element_type=F32)


def _grads(da, h1, h3):
    h1f = h1.astype(F32)
    h3f = h3.astype(F32)
    da = da.astype(BF16).astype(F32)
    s = jax.nn.sigmoid(h1f)
    silu = h1f * s
    a = (silu * h3f).astype(BF16)
    dh1 = (da * h3f * s * (1.0 + h1f * (1.0 - s))).astype(BF16)
    dh3 = (da * silu).astype(BF16)
    return a, dh1, dh3


def _scatter_rows(pos, gates, dy, nrows):
    t, d = dy.shape
    rb = 320

    def kernel(pos_ref, g_ref, dy_ref, o_ref, v_ref):
        @pl.when(pl.program_id(0) == 0)
        def _():
            v_ref[...] = (g_ref[...] * dy_ref[...].astype(F32)).astype(BF16)
        row = lax.broadcasted_iota(I32, (rb, t), 0) + pl.program_id(0) * rb
        oh = jnp.where(pos_ref[...] == row, 1.0, 0.0).astype(BF16)
        o_ref[...] = _dot(oh, v_ref[...]).astype(BF16)

    return pl.pallas_call(
        kernel, grid=(nrows // rb,),
        in_specs=[pl.BlockSpec((1, t), lambda i: (0, 0)),
                  pl.BlockSpec((t, 1), lambda i: (0, 0)),
                  pl.BlockSpec((t, d), lambda i: (0, 0))],
        out_specs=pl.BlockSpec((rb, d), lambda i: (i, 0)),
        out_shape=jax.ShapeDtypeStruct((nrows, d), BF16),
        scratch_shapes=[pltpu.VMEM((t, d), BF16)],
        compiler_params=_params(), name="scatter_rows",
        cost_estimate=_cost(2 * nrows * t * d, 2 * nrows * d * 2),
    )(pos.reshape(1, t), gates, dy)


def _gather_rows(pos, parts):
    t = pos.shape[0]
    k = len(parts)
    r, d = parts[0].shape
    tb = 512

    def kernel(pos_ref, *refs):
        o_ref = refs[k]
        acc = None
        p = pos_ref[...]
        for i in range(k):
            col = lax.broadcasted_iota(I32, (tb, r), 1) + i * r
            oh = jnp.where(p == col, 1.0, 0.0).astype(BF16)
            y = _dot(oh, refs[i][...])
            acc = y if acc is None else acc + y
        o_ref[...] = acc.astype(BF16)

    return pl.pallas_call(
        kernel, grid=(t // tb,),
        in_specs=[pl.BlockSpec((tb, 1), lambda i: (i, 0))] + [pl.BlockSpec((r, d), lambda i: (0, 0))] * k,
        out_specs=pl.BlockSpec((tb, d), lambda i: (i, 0)),
        out_shape=jax.ShapeDtypeStruct((t, d), BF16),
        compiler_params=_params(), name="gather_rows",
        cost_estimate=_cost(2 * k * r * t * d, 2 * k * r * d * 2),
    )(pos, *parts)


def _compact(tl, n, x):
    nt, tile, d = x.shape

    def kernel(tl_ref, n_ref, x_ref, o_ref, buf, sin, sout):
        n = n_ref[0]
        m = ((n + BT - 1) // BT) * BT

        @pl.loop(0, n)
        def _(i):
            pltpu.make_async_copy(x_ref.at[tl_ref[i]], buf.at[i], sin.at[i]).start()

        @pl.loop(n, m)
        def _(i):
            buf[i] = jnp.zeros((tile, d), x.dtype)

        @pl.loop(0, n)
        def _(i):
            pltpu.make_async_copy(x_ref.at[0], buf.at[i], sin.at[i]).wait()
            pltpu.make_async_copy(buf.at[i], o_ref.at[i], sout.at[i]).start()

        @pl.loop(n, m)
        def _(i):
            pltpu.make_async_copy(buf.at[i], o_ref.at[i], sout.at[i]).start()

        @pl.loop(0, m)
        def _(i):
            pltpu.make_async_copy(buf.at[i], o_ref.at[i], sout.at[i]).wait()

    return pl.pallas_call(
        kernel, in_specs=[SMEM, SMEM, HBM], out_specs=HBM,
        out_shape=jax.ShapeDtypeStruct(x.shape, x.dtype),
        scratch_shapes=[pltpu.VMEM(x.shape, x.dtype), pltpu.SemaphoreType.DMA((nt,)), pltpu.SemaphoreType.DMA((nt,))],
        compiler_params=_params(), name="compact",
        cost_estimate=_cost(1e6, 2 * x.size * 2),
    )(tl, n, x)


def _own_rows(tlx, tlk, n, half, dyd, h1, h3, w1t, w3t, w2t):
    nt, tile, d = dyd.shape
    f = h1.shape[2]
    fh = f // 2
    rows = BT * tile

    def kernel(tlx_ref, tlk_ref, n_ref, half_ref, dyd_ref, h1_ref, h3_ref, w1_hbm, w3_hbm, w2_hbm,
               dxd_ref, a_ref, dh1_ref, dh3_ref,
               w1v, w3v, w2v, gb, h1b, h3b, ob, hb, acc, zt, wsem, isem, osem, hsem, zsem):
        n = n_ref[0]
        nb = (n + BT - 1) // BT
        c0 = half_ref[0] * (fh // FC)
        nc = f // FC

        def tile_copies(b, slot, j):
            i = b * BT + j
            rs = pl.ds(j * tile, tile)
            return (pltpu.make_async_copy(dyd_ref.at[tlk_ref[i]], gb.at[slot, rs], isem.at[slot, 0, j]),
                    pltpu.make_async_copy(h1_ref.at[tlx_ref[i]], h1b.at[slot, rs], isem.at[slot, 1, j]),
                    pltpu.make_async_copy(h3_ref.at[tlx_ref[i]], h3b.at[slot, rs], isem.at[slot, 2, j]))

        def fetch(b, slot):
            for j in range(BT):
                @pl.when(b * BT + j < n)
                def _():
                    for c in tile_copies(b, slot, j):
                        c.start()

                @pl.when(b * BT + j >= n)
                def _():
                    rs = pl.ds(j * tile, tile)
                    gb[slot, rs] = jnp.zeros((tile, d), BF16)
                    h1b[slot, rs] = jnp.zeros((tile, f), BF16)
                    h3b[slot, rs] = jnp.zeros((tile, f), BF16)

        def arrive(b, slot):
            for j in range(BT):
                @pl.when(b * BT + j < n)
                def _():
                    for c in tile_copies(b, slot, j):
                        c.wait()

        def out_copy(b, slot, j):
            return pltpu.make_async_copy(ob.at[slot, pl.ds(j * tile, tile)], dxd_ref.at[tlk_ref[b * BT + j]],
                                         osem.at[slot, j])

        def half_copies(b, slot):
            rs = pl.ds(pl.multiple_of(b * rows, rows), rows)
            return [pltpu.make_async_copy(hb.at[slot, q], r.at[rs], hsem.at[slot, q])
                    for q, r in enumerate((a_ref, dh1_ref, dh3_ref))]

        def drain(b, slot):
            for j in range(BT):
                @pl.when(b * BT + j < n)
                def _():
                    out_copy(b, slot, j).wait()
            for c in half_copies(b, slot):
                c.wait()

        wcopies = [pltpu.make_async_copy(s, v, wsem.at[q])
                   for q, (s, v) in enumerate(((w2_hbm, w2v), (w1_hbm, w1v), (w3_hbm, w3v)))]

        @pl.when(nb > 0)
        def _():
            fetch(0, 0)
        for c in wcopies:
            c.start()
        zt[...] = jnp.zeros((tile, d), BF16)

        @pl.loop(n, nt)
        def _(i):
            pltpu.make_async_copy(zt, dxd_ref.at[tlk_ref[i]], zsem.at[i]).start()

        for c in wcopies:
            c.wait()

        @pl.loop(0, nb)
        def _(b):
            slot = lax.rem(b, 2)

            @pl.when(b + 1 < nb)
            def _():
                fetch(b + 1, 1 - slot)

            @pl.when(b >= 2)
            def _():
                drain(b - 2, slot)
            arrive(b, slot)

            def step(i, mine):
                c = lax.rem(c0 + i, nc)
                cs = pl.ds(pl.multiple_of(c * FC, FC), FC)
                da = _dot(gb[slot], w2v[:, cs])
                a, dh1, dh3 = _grads(da, h1b[slot, :, cs], h3b[slot, :, cs])
                y = _dot(dh1, w1v[cs, :]) + _dot(dh3, w3v[cs, :])
                if mine:
                    hs = pl.ds(pl.multiple_of(i * FC, FC), FC)
                    hb[slot, 0, :, hs] = a
                    hb[slot, 1, :, hs] = dh1
                    hb[slot, 2, :, hs] = dh3
                return y

            acc[...] = jnp.zeros((rows, d), F32)

            @pl.loop(0, nc // 2)
            def _(i):
                acc[...] += step(i, True)

            for c in half_copies(b, slot):
                c.start()

            @pl.loop(nc // 2, nc)
            def _(i):
                acc[...] += step(i, False)
            ob[slot] = acc[...].astype(BF16)
            for j in range(BT):
                @pl.when(b * BT + j < n)
                def _():
                    out_copy(b, slot, j).start()

        @pl.when(nb > 1)
        def _():
            drain(nb - 2, lax.rem(nb, 2))

        @pl.when(nb > 0)
        def _():
            drain(nb - 1, lax.rem(nb + 1, 2))

        @pl.loop(n, nt)
        def _(i):
            pltpu.make_async_copy(zt, dxd_ref.at[tlk_ref[i]], zsem.at[i]).wait()

    hshape = jax.ShapeDtypeStruct((nt * tile, fh), BF16)
    return pl.pallas_call(
        kernel, in_specs=[SMEM] * 4 + [HBM] * 6, out_specs=[HBM] * 4,
        out_shape=[jax.ShapeDtypeStruct(dyd.shape, BF16), hshape, hshape, hshape],
        scratch_shapes=[pltpu.VMEM((f, d), BF16), pltpu.VMEM((f, d), BF16), pltpu.VMEM((d, f), BF16),
                        pltpu.VMEM((2, rows, d), BF16), pltpu.VMEM((2, rows, f), BF16), pltpu.VMEM((2, rows, f), BF16),
                        pltpu.VMEM((2, rows, d), BF16), pltpu.VMEM((2, 3, rows, fh), BF16),
                        pltpu.VMEM((rows, d), F32), pltpu.VMEM((tile, d), BF16),
                        pltpu.SemaphoreType.DMA((3,)), pltpu.SemaphoreType.DMA((2, 3, BT)),
                        pltpu.SemaphoreType.DMA((2, BT)), pltpu.SemaphoreType.DMA((2, 3)),
                        pltpu.SemaphoreType.DMA((nt,))],
        compiler_params=_params(), name="own_rows",
        cost_estimate=_cost(2 * 1600 * d * f * 3, 5e7),
    )(tlx, tlk, n, half, dyd, h1, h3, w1t, w3t, w2t)


def _own_dw(n, xc, gc, a, dh1, dh3):
    nt, tile, d = xc.shape
    fh = a.shape[1]
    rows = BT * tile
    x2, g2 = xc.reshape(nt * tile, d), gc.reshape(nt * tile, d)

    def kernel(n_ref, x_ref, g_ref, a_ref, dh1_ref, dh3_ref, dw1_ref, dw3_ref, dw2_ref,
               xb, gb, hb, p1, p3, p2, isem, osem):
        nb = (n_ref[0] + BT - 1) // BT

        def copies(b, slot):
            rs = pl.ds(pl.multiple_of(b * rows, rows), rows)
            return [pltpu.make_async_copy(x_ref.at[rs], xb.at[slot], isem.at[slot, 0]),
                    pltpu.make_async_copy(g_ref.at[rs], gb.at[slot], isem.at[slot, 1])] + [
                    pltpu.make_async_copy(r.at[rs], hb.at[slot, q], isem.at[slot, 2 + q])
                    for q, r in enumerate((a_ref, dh1_ref, dh3_ref))]

        @pl.when(nb > 0)
        def _():
            for c in copies(0, 0):
                c.start()
        p1[...] = jnp.zeros(p1.shape, F32)
        p3[...] = jnp.zeros(p3.shape, F32)
        p2[...] = jnp.zeros(p2.shape, F32)

        @pl.loop(0, nb)
        def _(b):
            slot = lax.rem(b, 2)

            @pl.when(b + 1 < nb)
            def _():
                for c in copies(b + 1, 1 - slot):
                    c.start()
            for c in copies(b, slot):
                c.wait()
            xt = xb[slot].T

            @pl.loop(0, fh // FC)
            def _(i):
                cs = pl.ds(pl.multiple_of(i * FC, FC), FC)
                p1[:, cs] += _dot(xt, hb[slot, 1, :, cs])
                p3[:, cs] += _dot(xt, hb[slot, 2, :, cs])
                p2[cs, :] += _dot(hb[slot, 0, :, cs].T, gb[slot])

        outs = [pltpu.make_async_copy(p, o, osem.at[q])
                for q, (p, o) in enumerate(((p1, dw1_ref), (p3, dw3_ref), (p2, dw2_ref)))]
        for c in outs:
            c.start()
        for c in outs:
            c.wait()

    return pl.pallas_call(
        kernel, in_specs=[SMEM] + [HBM] * 5, out_specs=[HBM] * 3,
        out_shape=[jax.ShapeDtypeStruct((d, fh), F32), jax.ShapeDtypeStruct((d, fh), F32),
                   jax.ShapeDtypeStruct((fh, d), F32)],
        scratch_shapes=[pltpu.VMEM((2, rows, d), BF16), pltpu.VMEM((2, rows, d), BF16),
                        pltpu.VMEM((2, 3, rows, fh), BF16),
                        pltpu.VMEM((d, fh), F32), pltpu.VMEM((d, fh), F32), pltpu.VMEM((fh, d), F32),
                        pltpu.SemaphoreType.DMA((2, 5)), pltpu.SemaphoreType.DMA((3,))],
        compiler_params=_params(), name="own_dw",
        cost_estimate=_cost(2 * 1600 * d * fh * 3, 5e7),
    )(n, x2, g2, a, dh1, dh3)


def _peer_dw(n, half, xo, go, w1, w3, w2t, q1, q3, q2):
    nt, tile, d = xo.shape
    fh = q1.shape[1]
    rows = BT * tile

    def kernel(n_ref, half_ref, x_ref, g_ref, w1_hbm, w3_hbm, w2_hbm, q1_ref, q3_ref, q2_ref,
               dw1_ref, dw3_ref, dw2_ref, w1v, w3v, w2v, xb, gb, p1, p3, p2, wsem, isem, psem, osem):
        n = n_ref[0]
        nb = (n + BT - 1) // BT
        hs = pl.ds(pl.multiple_of(half_ref[0] * fh, fh), fh)

        def tile_copies(b, slot, j):
            i = b * BT + j
            rs = pl.ds(j * tile, tile)
            return (pltpu.make_async_copy(x_ref.at[i], xb.at[slot, rs], isem.at[slot, 0, j]),
                    pltpu.make_async_copy(g_ref.at[i], gb.at[slot, rs], isem.at[slot, 1, j]))

        def fetch(b, slot):
            for j in range(BT):
                @pl.when(b * BT + j < n)
                def _():
                    for c in tile_copies(b, slot, j):
                        c.start()

                @pl.when(b * BT + j >= n)
                def _():
                    rs = pl.ds(j * tile, tile)
                    xb[slot, rs] = jnp.zeros((tile, d), BF16)
                    gb[slot, rs] = jnp.zeros((tile, d), BF16)

        def arrive(b, slot):
            for j in range(BT):
                @pl.when(b * BT + j < n)
                def _():
                    for c in tile_copies(b, slot, j):
                        c.wait()

        wcopies = [pltpu.make_async_copy(s.at[:, hs], v, wsem.at[q])
                   for q, (s, v) in enumerate(((w1_hbm, w1v), (w3_hbm, w3v), (w2_hbm, w2v)))]
        pcopies = [pltpu.make_async_copy(s, v, psem.at[q])
                   for q, (s, v) in enumerate(((q1_ref, p1), (q3_ref, p3), (q2_ref, p2)))]
        for c in wcopies:
            c.start()

        @pl.when(nb > 0)
        def _():
            fetch(0, 0)
        for c in pcopies:
            c.start()
        for c in wcopies:
            c.wait()
        for c in pcopies:
            c.wait()

        @pl.loop(0, nb)
        def _(b):
            slot = lax.rem(b, 2)

            @pl.when(b + 1 < nb)
            def _():
                fetch(b + 1, 1 - slot)
            arrive(b, slot)
            xt = xb[slot].T

            @pl.loop(0, fh // FC)
            def _(i):
                cs = pl.ds(pl.multiple_of(i * FC, FC), FC)
                h1 = _dot(xb[slot], w1v[:, cs]).astype(BF16)
                h3 = _dot(xb[slot], w3v[:, cs]).astype(BF16)
                da = _dot(gb[slot], w2v[:, cs])
                a, dh1, dh3 = _grads(da, h1, h3)
                p1[:, cs] += _dot(xt, dh1)
                p3[:, cs] += _dot(xt, dh3)
                p2[cs, :] += _dot(a.T, gb[slot])

        outs = [pltpu.make_async_copy(p, o, osem.at[q])
                for q, (p, o) in enumerate(((p1, dw1_ref), (p3, dw3_ref), (p2, dw2_ref)))]
        for c in outs:
            c.start()
        for c in outs:
            c.wait()

    return pl.pallas_call(
        kernel, in_specs=[SMEM] * 2 + [HBM] * 8, out_specs=[HBM] * 3,
        out_shape=[jax.ShapeDtypeStruct((d, fh), F32), jax.ShapeDtypeStruct((d, fh), F32),
                   jax.ShapeDtypeStruct((fh, d), F32)],
        scratch_shapes=[pltpu.VMEM((d, fh), BF16)] * 3 + [
                        pltpu.VMEM((2, rows, d), BF16), pltpu.VMEM((2, rows, d), BF16),
                        pltpu.VMEM((d, fh), F32), pltpu.VMEM((d, fh), F32), pltpu.VMEM((fh, d), F32),
                        pltpu.SemaphoreType.DMA((3,)), pltpu.SemaphoreType.DMA((2, 2, BT)),
                        pltpu.SemaphoreType.DMA((3,)), pltpu.SemaphoreType.DMA((3,))],
        compiler_params=_params(), name="peer_dw",
        cost_estimate=_cost(2 * 1600 * d * fh * 6, 5e7),
    )(n, half, xo, go, w1, w3, w2t, q1, q3, q2)


def solution(mesh):
    ne = mesh.shape['expert']
    nd = mesh.shape['data']
    tok = P(('data', 'expert'), None)
    buf = P(('data', 'expert'), None, None)
    wsp = P('expert', None, None)
    zswap = [(i, nd - 1 - i) for i in range(nd)]

    def body(dy, gates, topk_idx, slot, yd, xd, h1, h3, w1, w3, w2):
        d = dy.shape[1]
        cap = xd.shape[1] // ne
        f = w1.shape[2]
        nt = xd.shape[1] // TILE
        tps = cap // TILE
        me = lax.axis_index('expert')
        grp = lax.axis_index('data')
        half = grp.astype(I32).reshape(1)

        x4 = xd.reshape(nt, TILE, d)
        occ = jnp.any(x4 != 0, axis=(1, 2)).astype(I32)
        n = jnp.sum(occ)
        before = jnp.cumsum(occ) - occ
        ids = jnp.arange(nt, dtype=I32)
        place = jnp.where(occ > 0, before, n + ids - before)
        tlx = jnp.sum(jnp.where(place[None, :] == ids[:, None], ids[None, :], 0), axis=1)
        tlk = ((tlx // tps) ^ me) * tps + tlx % tps
        n = n.reshape(1)
        npeer = lax.ppermute(n, 'data', zswap)

        def swap_rows(c):
            return lax.ppermute(c, 'data', zswap)

        xc = _compact(tlx, n, x4)
        xo = swap_rows(xc)

        pos = jnp.where(slot >= 0, (topk_idx ^ me) * cap + slot, -1)
        send = _scatter_rows(pos, gates, dy, ne * cap).reshape(ne, cap, d)
        xor = lambda k: [(i, i ^ k) for i in range(ne)]
        dyd = jnp.concatenate([send[:1]] + [lax.ppermute(send[k:k + 1], 'expert', xor(k)) for k in range(1, ne)], axis=0)
        dyd = dyd.reshape(nt, TILE, d)
        gc = _compact(tlk, n, dyd)
        go = swap_rows(gc)

        w1t, w3t, w2t = w1[0].T, w3[0].T, w2[0].T
        dxd, a, dh1, dh3 = _own_rows(tlx, tlk, n, half, dyd, h1.reshape(nt, TILE, f), h3.reshape(nt, TILE, f),
                                     w1t, w3t, w2t)
        out = dxd.reshape(ne, cap, d)
        back = [out[0]] + [lax.ppermute(out[k], 'expert', xor(k)) for k in range(1, ne)]
        q1, q3, q2 = _own_dw(n, xc, gc, a, dh1, dh3)
        dg = jnp.einsum('tkd,td->tk', yd, dy, preferred_element_type=F32)
        dx = _gather_rows(pos, back)
        dw1, dw3, dw2 = _peer_dw(npeer, half, xo, go, w1[0], w3[0], w2t, q1, q3, q2)
        return dx, dg, dw1[None], dw3[None], dw2[None]

    return jax.shard_map(body, mesh=mesh,
                         in_specs=(tok, tok, tok, tok, buf, buf, buf, buf, wsp, wsp, wsp),
                         out_specs=(tok, tok, P('expert', None, 'data'), P('expert', None, 'data'), P('expert', 'data', None)),
                         check_vma=False)
```

```python
import jax
import jax.numpy as jnp
from jax import lax
from jax.experimental import pallas as pl
from jax.experimental.pallas import tpu as pltpu
from jax.sharding import PartitionSpec as P


F32 = jnp.float32
BF16 = jnp.bfloat16
I32 = jnp.int32


TILE = 64
BT = 8
FC = 768
VMEM_LIMIT = 62 * 1024 * 1024

ANY = pl.BlockSpec(memory_space=pl.ANY)
HBM = pl.BlockSpec(memory_space=pltpu.HBM)
SMEM = pl.BlockSpec(memory_space=pltpu.SMEM)


def _params(**kw):
    return pltpu.CompilerParams(vmem_limit_bytes=VMEM_LIMIT, **kw)


def _cost(flops, nbytes):
    return pl.CostEstimate(flops=int(flops), bytes_accessed=int(nbytes), transcendentals=0)


def _dot(a, b):
    return jnp.dot(a, b, preferred_element_type=F32)


def _grads(da, h1, h3):
    h1f = h1.astype(F32)
    h3f = h3.astype(F32)
    da = da.astype(BF16).astype(F32)
    s = jax.nn.sigmoid(h1f)
    silu = h1f * s
    a = (silu * h3f).astype(BF16)
    dh1 = ((da * h3f) * (s + silu * (1.0 - s))).astype(BF16)
    dh3 = (da * silu).astype(BF16)
    return a, dh1, dh3


def _scatter_rows(pos, gates, dy, ks, cap):
    t, d = dy.shape
    k = len(ks)

    def kernel(pos_ref, g_ref, dy_ref, *refs):
        outs, v_ref, ob, sem = refs[:k], refs[k], refs[k + 1], refs[k + 2]
        v_ref[...] = (g_ref[...] * dy_ref[...].astype(F32)).astype(BF16)

        @pl.loop(0, k)
        def _(q):
            base = sum(jnp.where(q == p, ks[p] * cap, 0) for p in range(k))
            row = lax.broadcasted_iota(I32, (cap, t), 0) + base
            oh = jnp.where(pos_ref[...] == row, 1.0, 0.0).astype(BF16)
            ob[q] = _dot(oh, v_ref[...]).astype(BF16)
            for p in range(k):
                @pl.when(q == p)
                def _():
                    pltpu.make_async_copy(ob.at[p], outs[p], sem.at[p]).start()

        for p in range(k):
            pltpu.make_async_copy(ob.at[p], outs[p], sem.at[p]).wait()

    vm = pl.BlockSpec(memory_space=pltpu.VMEM)
    return pl.pallas_call(
        kernel, in_specs=[vm] * 3, out_specs=[HBM] * k,
        out_shape=[jax.ShapeDtypeStruct((cap, d), BF16)] * k,
        scratch_shapes=[pltpu.VMEM((t, d), BF16), pltpu.VMEM((k, cap, d), BF16), pltpu.SemaphoreType.DMA((k,))],
        compiler_params=_params(), name="scatter_rows",
        cost_estimate=_cost(2 * k * cap * t * d, 2 * k * cap * d * 2),
    )(pos, gates, dy)


def _gather_rows(pos, parts):
    t = pos.shape[0]
    k = len(parts)
    r, d = parts[0].shape
    tb = 512

    def kernel(pos_ref, *refs):
        ins, o_ref, src, sem = refs[:k], refs[k], refs[k + 1], refs[k + 2]

        @pl.when(pl.program_id(0) == 0)
        def _():
            for q in range(k):
                pltpu.make_async_copy(ins[q], src.at[pl.ds(q * r, r)], sem.at[q]).start()
            for q in range(k):
                pltpu.make_async_copy(ins[q], src.at[pl.ds(q * r, r)], sem.at[q]).wait()

        col = lax.broadcasted_iota(I32, (tb, k * r), 1)
        oh = jnp.where(pos_ref[...] == col, 1.0, 0.0).astype(BF16)
        o_ref[...] = _dot(oh, src[...]).astype(BF16)

    return pl.pallas_call(
        kernel, grid=(t // tb,),
        in_specs=[pl.BlockSpec((tb, 1), lambda i: (i, 0))] + [HBM] * k,
        out_specs=pl.BlockSpec((tb, d), lambda i: (i, 0)),
        out_shape=jax.ShapeDtypeStruct((t, d), BF16),
        scratch_shapes=[pltpu.VMEM((k * r, d), BF16), pltpu.SemaphoreType.DMA((k,))],
        compiler_params=_params(), name="gather_rows",
        cost_estimate=_cost(2 * k * r * t * d, 2 * k * r * d * 2),
    )(pos, *parts)


def _own_rows(rng, tl, meta, first, gs, h1, h3, w1t, w3t, w2t, halves, nblk):
    ng = len(gs)
    cap, d = gs[0].shape
    _, tile, f = h1.shape
    tps = cap // tile
    fh = f // 2
    rows = BT * tile
    fc = 512
    nc = f // fc
    alias = halves is not None

    def kernel(rng_ref, tl_ref, meta_ref, *refs):
        g_refs, refs = refs[:ng], refs[ng:]
        h1_ref, h3_ref, w1_hbm, w3_hbm, w2_hbm = refs[:5]
        refs = refs[5 + (3 if alias else 0):]
        dxd_refs, refs = refs[:ng], refs[ng:]
        (a_ref, dh1_ref, dh3_ref, w13v, w2v, gall, h1b, h3b, oall, hb, acc,
         wsem, gsem, isem, osem, hsem) = refs
        b0, b1 = rng_ref[0], rng_ref[1]
        half, me = meta_ref[0], meta_ref[1]
        c0 = half * (nc // 2)

        def src_tile(t):
            return lax.bitwise_xor(t // tps, me) * tps + lax.rem(t, tps)

        def tile_copies(b, slot, j):
            t = src_tile(tl_ref[b * BT + j])
            rs = pl.ds(j * tile, tile)
            return (pltpu.make_async_copy(h1_ref.at[t], h1b.at[slot, rs], isem.at[slot, 0, j]),
                    pltpu.make_async_copy(h3_ref.at[t], h3b.at[slot, rs], isem.at[slot, 1, j]))

        def fetch(b, slot):
            for j in range(BT):
                @pl.when(tl_ref[b * BT + j] >= 0)
                def _():
                    for c in tile_copies(b, slot, j):
                        c.start()

                @pl.when(tl_ref[b * BT + j] < 0)
                def _():
                    rs = pl.ds(j * tile, tile)
                    h1b[slot, rs] = jnp.zeros((tile, f), BF16)
                    h3b[slot, rs] = jnp.zeros((tile, f), BF16)

        def arrive(b, slot):
            for j in range(BT):
                @pl.when(tl_ref[b * BT + j] >= 0)
                def _():
                    for c in tile_copies(b, slot, j):
                        c.wait()

        def half_copies(b):
            rs = pl.ds(pl.multiple_of(b * rows, rows), rows)
            return [pltpu.make_async_copy(hb.at[q], r.at[rs], hsem.at[q])
                    for q, r in enumerate((a_ref, dh1_ref, dh3_ref))]

        gcopies = [pltpu.make_async_copy(g_refs[q], gall.at[pl.ds(q * cap, cap)], gsem.at[q]) for q in range(ng)]

        def wcopies(i, parts=(0, 1, 2)):
            c = lax.rem(c0 + i, nc)
            cs = pl.ds(pl.multiple_of(c * fc, fc), fc)
            return [pltpu.make_async_copy(w2_hbm.at[:, cs], w2v.at[:, cs], wsem.at[i, 0]) if q == 0 else
                    pltpu.make_async_copy((w1_hbm, w3_hbm)[q - 1].at[cs], w13v.at[c, pl.ds((q - 1) * fc, fc)],
                                          wsem.at[i, q])
                    for q in parts]

        for c in gcopies + wcopies(0, (0,)):
            c.start()

        @pl.when(b0 < b1)
        def _():
            fetch(b0, 0)

        for c in wcopies(0, (1, 2)):
            c.start()
        for i in range(1, nc):
            for c in wcopies(i):
                c.start()
        oall[...] = jnp.zeros(oall.shape, BF16)
        for c in gcopies:
            c.wait()

        def weights(b, i, part):
            @pl.when(b == b0)
            def _():
                for c in wcopies(i, part):
                    c.wait()

        @pl.loop(b0, b1)
        def _(b):
            slot = lax.rem(b - b0, 2)

            @pl.when(b + 1 < b1)
            def _():
                fetch(b + 1, 1 - slot)

            g = jnp.concatenate(
                [jnp.where(tl_ref[b * BT + j] >= 0,
                           gall[pl.ds(pl.multiple_of(jnp.maximum(tl_ref[b * BT + j] - first * tps, 0) * tile, tile), tile)],
                           jnp.zeros((tile, d), BF16)) for j in range(BT)], axis=0)
            arrive(b, slot)

            @pl.when(b > b0)
            def _():
                for c in half_copies(b - 1):
                    c.wait()

            def col(i):
                c = lax.rem(c0 + i, nc)
                return c, pl.ds(pl.multiple_of(c * fc, fc), fc)

            weights(b, 0, (0,))
            da = _dot(g, w2v[:, col(0)[1]])
            for i in range(nc):
                c, cs = col(i)
                weights(b, i, (1, 2))
                if i + 1 < nc:
                    weights(b, i + 1, (0,))
                nxt = _dot(g, w2v[:, col(i + 1)[1]]) if i + 1 < nc else None
                a, dh1, dh3 = _grads(da, h1b[slot, :, cs], h3b[slot, :, cs])
                if i < nc // 2:
                    hs = pl.ds(i * fc, fc)
                    hb[0, :, hs] = a
                    hb[1, :, hs] = dh1
                    hb[2, :, hs] = dh3
                y = _dot(jnp.concatenate([dh1, dh3], axis=1), w13v[c])
                if i == 0:
                    acc[...] = y
                else:
                    acc[...] += y
                da = nxt
                if i == nc // 2 - 1:
                    for cp in half_copies(b):
                        cp.start()
            for j in range(BT):
                @pl.when(tl_ref[b * BT + j] >= 0)
                def _():
                    t = tl_ref[b * BT + j] - first * tps
                    oall[pl.ds(pl.multiple_of(t * tile, tile), tile)] = acc[pl.ds(j * tile, tile)].astype(BF16)

        @pl.when(b0 >= b1)
        def _():
            for i in range(nc):
                for c in wcopies(i):
                    c.wait()

        outs = [pltpu.make_async_copy(oall.at[pl.ds(q * cap, cap)], dxd_refs[q], osem.at[q]) for q in range(ng)]
        for c in outs:
            c.start()

        @pl.when(b0 < b1)
        def _():
            for c in half_copies(b1 - 1):
                c.wait()

        for c in outs:
            c.wait()

    hshape = jax.ShapeDtypeStruct((nblk * rows, fh), BF16)
    base = 3 + ng + 5
    return pl.pallas_call(
        kernel, in_specs=[SMEM] * 3 + [HBM] * (ng + 5 + (3 if alias else 0)), out_specs=[HBM] * (ng + 3),
        out_shape=[jax.ShapeDtypeStruct((cap, d), BF16)] * ng + [hshape] * 3,
        input_output_aliases={base + q: ng + q for q in range(3)} if alias else {},
        scratch_shapes=[pltpu.VMEM((nc, 2 * fc, d), BF16), pltpu.VMEM((d, f), BF16),
                        pltpu.VMEM((ng * cap, d), BF16), pltpu.VMEM((2, rows, f), BF16), pltpu.VMEM((2, rows, f), BF16),
                        pltpu.VMEM((ng * cap, d), BF16), pltpu.VMEM((3, rows, fh), BF16),
                        pltpu.VMEM((rows, d), F32),
                        pltpu.SemaphoreType.DMA((nc, 3)), pltpu.SemaphoreType.DMA((ng,)),
                        pltpu.SemaphoreType.DMA((2, 2, BT)), pltpu.SemaphoreType.DMA((ng,)),
                        pltpu.SemaphoreType.DMA((3,))],
        compiler_params=_params(), name="own_rows",
        cost_estimate=_cost(2 * 200 * ng * d * f * 3, 5e7),
    )(rng, tl, meta, *gs, h1, h3, w1t, w3t, w2t, *(halves if alias else ()))


def _dw(rng, tl, meta, first, gs, x, own, peer, sums):
    ng = len(gs)
    cap, d = gs[0].shape
    _, tile, _ = x.shape
    tps = cap // tile
    fh = own[0].shape[1] if own else peer[0].shape[1] // 2
    rows = BT * tile
    fc = FC
    nc = fh // fc
    nadd = 3 if sums else 0
    mb = -(-ng * tps // BT)
    if own:
        mb += 1

    def kernel(rng_ref, tl_ref, meta_ref, *refs):
        g_refs, x_ref, refs = refs[:ng], refs[ng], refs[ng + 1:]
        s_refs, q_refs, o_refs = refs[:3], refs[3:3 + nadd], refs[3 + nadd:6 + nadd]
        (gall, xb, xt, gb, sv, p1, p3, p2, gsem, xsem, ssem, psem, osem) = refs[6 + nadd:]
        b0, b1 = rng_ref[0], rng_ref[1]
        half, me = meta_ref[0], meta_ref[1]

        def xcopy(b, j):
            t = tl_ref[b * BT + j]
            t = lax.bitwise_xor(t // tps, me) * tps + lax.rem(t, tps)
            return pltpu.make_async_copy(x_ref.at[t], xb.at[b - b0, pl.ds(j * tile, tile)], xsem.at[b - b0, j])

        gcopies = [pltpu.make_async_copy(g_refs[q], gall.at[pl.ds(q * cap, cap)], gsem.at[q]) for q in range(ng)]

        def pcopies(c, slot):
            cs = pl.ds(pl.multiple_of(c * fc, fc), fc)
            views = ((p1, (slice(None), cs)), (p3, (slice(None), cs)), (p2, (cs, slice(None))))
            return [pltpu.make_async_copy(q.at[ix], p.at[slot], psem.at[slot, r])
                    for r, (q, (p, ix)) in enumerate(zip(q_refs, views))]

        def ocopies(c, slot):
            cs = pl.ds(pl.multiple_of(c * fc, fc), fc)
            views = ((p1, (slice(None), cs)), (p3, (slice(None), cs)), (p2, (cs, slice(None))))
            return [pltpu.make_async_copy(p.at[slot], o.at[ix], osem.at[slot, r])
                    for r, (o, (p, ix)) in enumerate(zip(o_refs, views))]

        def wcopies(c, slot):
            cs = pl.ds(pl.multiple_of(half * fh + c * fc, fc), fc)
            return [pltpu.make_async_copy(s.at[:, cs], sv.at[slot, r], ssem.at[slot, r]) for r, s in enumerate(s_refs)]

        def scopies(c, b, slot):
            rs = pl.ds(pl.multiple_of(b * rows, rows), rows)
            cs = pl.ds(pl.multiple_of(c * fc, fc), fc)
            return [pltpu.make_async_copy(s.at[rs, cs], sv.at[slot, r], ssem.at[slot, r]) for r, s in enumerate(s_refs)]

        for c in gcopies:
            c.start()

        @pl.loop(b0, b1)
        def _(b):
            for j in range(BT):
                @pl.when(tl_ref[b * BT + j] >= 0)
                def _():
                    xcopy(b, j).start()

                @pl.when(tl_ref[b * BT + j] < 0)
                def _():
                    xb[b - b0, pl.ds(j * tile, tile)] = jnp.zeros((tile, d), BF16)

        if peer:
            for cp in wcopies(0, 0):
                cp.start()
        if sums:
            for cp in pcopies(0, 0):
                cp.start()
        if own:
            @pl.when(b0 < b1)
            def _():
                for cp in scopies(0, b0, 0):
                    cp.start()
        for c in gcopies:
            c.wait()

        @pl.loop(b0, b1)
        def _(b):
            for j in range(BT):
                @pl.when(tl_ref[b * BT + j] >= 0)
                def _():
                    xcopy(b, j).wait()
                    t = tl_ref[b * BT + j] - first * tps
                    gb[b - b0, pl.ds(j * tile, tile)] = gall[pl.ds(pl.multiple_of(t * tile, tile), tile)]

                @pl.when(tl_ref[b * BT + j] < 0)
                def _():
                    gb[b - b0, pl.ds(j * tile, tile)] = jnp.zeros((tile, d), BF16)
            xt[b - b0] = xb[b - b0].T

        @pl.loop(0, nc)
        def _(c):
            ps = lax.rem(c, 2)
            if peer:
                @pl.when(c + 1 < nc)
                def _():
                    for cp in wcopies(c + 1, 1 - ps):
                        cp.start()

                for cp in wcopies(c, ps):
                    cp.wait()

            @pl.when(c >= 1)
            def _():
                for cp in ocopies(c - 1, 1 - ps):
                    cp.wait()

            if sums:
                @pl.when(c + 1 < nc)
                def _():
                    for cp in pcopies(c + 1, 1 - ps):
                        cp.start()

                for cp in pcopies(c, ps):
                    cp.wait()
            else:
                p1[ps] = jnp.zeros((d, fc), F32)
                p3[ps] = jnp.zeros((d, fc), F32)
                p2[ps] = jnp.zeros((fc, d), F32)

            @pl.loop(b0, b1)
            def _(b):
                i = b - b0
                if own:
                    slot = lax.rem(c * (b1 - b0) + i, 2)

                    @pl.when(b + 1 < b1)
                    def _():
                        for cp in scopies(c, b + 1, 1 - slot):
                            cp.start()

                    @pl.when((b + 1 == b1) & (c + 1 < nc))
                    def _():
                        for cp in scopies(c + 1, b0, 1 - slot):
                            cp.start()

                    for cp in scopies(c, b, slot):
                        cp.wait()
                    a, dh1, dh3 = sv[slot, 0], sv[slot, 1], sv[slot, 2]
                else:
                    h1 = _dot(xb[i], sv[ps, 0]).astype(BF16)
                    h3 = _dot(xb[i], sv[ps, 1]).astype(BF16)
                    da = _dot(gb[i], sv[ps, 2])
                    a, dh1, dh3 = _grads(da, h1, h3)
                p1[ps] += _dot(xt[i], dh1)
                p3[ps] += _dot(xt[i], dh3)
                p2[ps] += _dot(a.T, gb[i])

            for cp in ocopies(c, ps):
                cp.start()

        for cp in ocopies(nc - 1, (nc - 1) % 2):
            cp.wait()

    srows = rows if own else d
    outs = [jax.ShapeDtypeStruct((d, fh), F32), jax.ShapeDtypeStruct((d, fh), F32), jax.ShapeDtypeStruct((fh, d), F32)]
    return pl.pallas_call(
        kernel, in_specs=[SMEM] * 3 + [HBM] * (ng + 4 + nadd), out_specs=[HBM] * 3, out_shape=outs,
        scratch_shapes=[pltpu.VMEM((ng * cap, d), BF16), pltpu.VMEM((mb, rows, d), BF16), pltpu.VMEM((mb, d, rows), BF16),
                        pltpu.VMEM((mb, rows, d), BF16), pltpu.VMEM((2, 3, srows, fc), BF16),
                        pltpu.VMEM((2, d, fc), F32), pltpu.VMEM((2, d, fc), F32), pltpu.VMEM((2, fc, d), F32),
                        pltpu.SemaphoreType.DMA((ng,)), pltpu.SemaphoreType.DMA((mb, BT)),
                        pltpu.SemaphoreType.DMA((2, 3)), pltpu.SemaphoreType.DMA((2, 3)), pltpu.SemaphoreType.DMA((2, 3))],
        compiler_params=_params(), name="own_dw" if own else "peer_dw",
        cost_estimate=_cost(2 * 200 * ng * d * fh * (3 if own else 6), 5e7),
    )(rng, tl, meta, *gs, x, *(own or peer), *(sums or ()))


def solution(mesh):
    ne = mesh.shape['expert']
    nd = mesh.shape['data']
    tok = P(('data', 'expert'), None)
    buf = P(('data', 'expert'), None, None)
    wsp = P('expert', None, None)
    zswap = [(i, nd - 1 - i) for i in range(nd)]
    ka = ne * 3 // 4
    cuts = (0, 3, ka, ne)
    groups = ((2, 4), (3, 5), (6, 7), (1, 0))

    def run(dy, gates, topk_idx, slot, yd, xd, h1, h3, w1, w3, w2):
        t, d = dy.shape
        cap = xd.shape[1] // ne
        f = w1.shape[2]
        nt = xd.shape[1] // TILE
        tps = cap // TILE
        me = lax.axis_index('expert').astype(I32)
        grp = lax.axis_index('data').astype(I32)
        meta = jnp.stack([grp, me])
        xor = lambda k: [(i, i ^ k) for i in range(ne)]
        swap = lambda v: lax.ppermute(v, 'data', zswap)

        x4 = xd.reshape(nt, TILE, d)
        xo = swap(x4)

        rpos = jnp.where(slot.reshape(1, t) >= 0, (topk_idx.reshape(1, t) ^ me) * cap + slot.reshape(1, t), -1)
        send = [None] * ne
        for ks in groups:
            for k, v in zip(ks, _scatter_rows(rpos, gates, dy, ks, cap)):
                send[k] = v
        dyd = [send[0]]
        for k in range(1, ne):
            dyd.append(lax.ppermute(send[k], 'expert', xor(k)))
        dyo = []
        for k in range(ne):
            dyo.append(swap(dyd[k]))

        occ = jnp.any(x4 != 0, axis=(1, 2)).astype(I32)
        occo = swap(occ)
        ids = jnp.arange(nt, dtype=I32)
        nblk = -(-ka * tps // BT) + -(-(ne - ka) * tps // BT)
        cells = jnp.arange((nblk + 1) * BT, dtype=I32)

        def lists(occ, cuts):
            src = ((ids // tps) ^ me) * tps + ids % tps
            ok = jnp.sum(jnp.where(src[:, None] == ids[None, :], occ[None, :], 0), axis=1)
            part = sum((ids >= c * tps).astype(I32) for c in cuts[1:-1])
            nums = jnp.arange(len(cuts) - 1, dtype=I32)
            cnt = jnp.sum(jnp.where(part[None, :] == nums[:, None], ok[None, :], 0), axis=1)
            blk = (cnt + BT - 1) // BT
            end = jnp.sum(jnp.where(nums[None, :] <= nums[:, None], blk[None, :], 0), axis=1)
            same = (part[None, :] == part[:, None]) & (ids[None, :] < ids[:, None])
            before = jnp.sum(jnp.where(same, ok[None, :], 0), axis=1)
            start = jnp.sum(jnp.where(nums[None, :] == part[:, None], (end - blk)[None, :], 0), axis=1)
            place = jnp.where(ok > 0, before + start * BT, -1)
            tl = jnp.sum(jnp.where(place[None, :] == cells[:, None], ids[None, :] + 1, 0), axis=1) - 1
            return tl, jnp.concatenate([jnp.zeros((1,), I32), end])

        tl, bnd = lists(occ, (0, ka, ne))
        tlo, bndo = lists(occo, cuts)

        w1t, w3t, w2t = w1[0].T, w3[0].T, w2[0].T
        h14, h34 = h1.reshape(nt, TILE, f), h3.reshape(nt, TILE, f)
        *da, ha, hd1, hd3 = _own_rows(bnd[0:2], tl, meta, 0, dyd[:ka], h14, h34, w1t, w3t, w2t, None, nblk)
        back = [da[0]]
        for k in range(1, ka):
            back.append(lax.ppermute(da[k], 'expert', xor(k)))
        *db, ha, hd1, hd3 = _own_rows(bnd[1:3], tl, meta, ka, dyd[ka:], h14, h34, w1t, w3t, w2t, (ha, hd1, hd3), nblk)
        for k in range(ka, ne):
            back.append(lax.ppermute(db[k - ka], 'expert', xor(k)))
        sums = _dw(jnp.stack([bnd[0], bnd[2]]), tl, meta, 0, dyd, x4, (ha, hd1, hd3), None, None)
        dg = jnp.einsum('tkd,td->tk', yd, dy, preferred_element_type=F32)
        dx = _gather_rows(rpos.reshape(t, 1), back)
        peer = (w1[0], w3[0], w2t)
        for p in range(len(cuts) - 1):
            sums = _dw(bndo[p:p + 2], tlo, meta, cuts[p], dyo[cuts[p]:cuts[p + 1]], xo, None, peer, sums)
        dw1, dw3, dw2 = sums
        return dx, dg, dw1[None], dw3[None], dw2[None]


    return jax.shard_map(run, mesh=mesh,
                         in_specs=(tok, tok, tok, tok, buf, buf, buf, buf, wsp, wsp, wsp),
                         out_specs=(tok, tok, P('expert', None, 'data'), P('expert', None, 'data'), P('expert', 'data', None)),
                         check_vma=False)
```

```python
import jax
import jax.numpy as jnp
from jax import lax
from jax.experimental import pallas as pl
from jax.experimental.pallas import tpu as pltpu
from jax.sharding import PartitionSpec as P


F32 = jnp.float32
BF16 = jnp.bfloat16
I32 = jnp.int32


TILE = 64
BT = 4
FC = 768
VMEM_LIMIT = 62 * 1024 * 1024

ANY = pl.BlockSpec(memory_space=pl.ANY)
HBM = pl.BlockSpec(memory_space=pltpu.HBM)
SMEM = pl.BlockSpec(memory_space=pltpu.SMEM)


def _params(**kw):
    return pltpu.CompilerParams(vmem_limit_bytes=VMEM_LIMIT, **kw)


def _cost(flops, nbytes):
    return pl.CostEstimate(flops=int(flops), bytes_accessed=int(nbytes), transcendentals=0)


def _dot(a, b):
    return jnp.dot(a, b, preferred_element_type=F32)


def _dot_nt(a, b):
    return lax.dot_general(a, b, (((1,), (1,)), ((), ())), preferred_element_type=F32)


def _grads(da, h1, h3):
    h1f = h1.astype(F32)
    h3f = h3.astype(F32)
    da = da.astype(BF16).astype(F32)
    s = jax.nn.sigmoid(h1f)
    silu = h1f * s
    a = (silu * h3f).astype(BF16)
    dh1 = ((da * h3f) * (s + silu * (1.0 - s))).astype(BF16)
    dh3 = (da * silu).astype(BF16)
    return a, dh1, dh3


def _scatter_rows(topk, slot, gates, dy, me, ks, cap):
    t, d = dy.shape
    k = len(ks)

    def kernel(meta_ref, e_ref, s_ref, g_ref, dy_ref, *refs):
        outs, v_ref, ob, sem = refs[:k], refs[k], refs[k + 1], refs[k + 2]
        v_ref[...] = (g_ref[...] * dy_ref[...].astype(F32)).astype(BF16)

        @pl.loop(0, k)
        def _(q):
            kq = sum(jnp.where(q == p, ks[p], 0) for p in range(k))
            pos = jnp.where(e_ref[...] == lax.bitwise_xor(kq, meta_ref[1]), s_ref[...], -1)
            row = lax.broadcasted_iota(I32, (cap, t), 0)
            oh = jnp.where(pos == row, 1.0, 0.0).astype(BF16)
            ob[q] = _dot(oh, v_ref[...]).astype(BF16)
            for p in range(k):
                @pl.when(q == p)
                def _():
                    pltpu.make_async_copy(ob.at[p], outs[p], sem.at[p]).start()

        for p in range(k):
            pltpu.make_async_copy(ob.at[p], outs[p], sem.at[p]).wait()

    vm = pl.BlockSpec(memory_space=pltpu.VMEM)
    return pl.pallas_call(
        kernel, in_specs=[SMEM] + [vm] * 4, out_specs=[HBM] * k,
        out_shape=[jax.ShapeDtypeStruct((cap, d), BF16)] * k,
        scratch_shapes=[pltpu.VMEM((t, d), BF16), pltpu.VMEM((k, cap, d), BF16), pltpu.SemaphoreType.DMA((k,))],
        compiler_params=_params(), name="scatter_rows",
        cost_estimate=_cost(2 * k * cap * t * d, 2 * k * cap * d * 2),
    )(me, topk, slot, gates, dy)


def _gather_rows(pos, parts):
    t = pos.shape[0]
    k = len(parts)
    r, d = parts[0].shape
    tb = 512

    def kernel(pos_ref, *refs):
        ins, o_ref, src, sem = refs[:k], refs[k], refs[k + 1], refs[k + 2]

        @pl.when(pl.program_id(0) == 0)
        def _():
            for q in range(k):
                pltpu.make_async_copy(ins[q], src.at[pl.ds(q * r, r)], sem.at[q]).start()
            for q in range(k):
                pltpu.make_async_copy(ins[q], src.at[pl.ds(q * r, r)], sem.at[q]).wait()

        col = lax.broadcasted_iota(I32, (tb, k * r), 1)
        oh = jnp.where(pos_ref[...] == col, 1.0, 0.0).astype(BF16)
        o_ref[...] = _dot(oh, src[...]).astype(BF16)

    return pl.pallas_call(
        kernel, grid=(t // tb,),
        in_specs=[pl.BlockSpec((tb, 1), lambda i: (i, 0))] + [HBM] * k,
        out_specs=pl.BlockSpec((tb, d), lambda i: (i, 0)),
        out_shape=jax.ShapeDtypeStruct((t, d), BF16),
        scratch_shapes=[pltpu.VMEM((k * r, d), BF16), pltpu.SemaphoreType.DMA((k,))],
        compiler_params=_params(), name="gather_rows",
        cost_estimate=_cost(2 * k * r * t * d, 2 * k * r * d * 2),
    )(pos, *parts)


def _own_rows(rng, tl, meta, first, gs, h1, h3, w1, w3, w2, halves, nblk, at):
    ng = len(gs)
    cap, d = gs[0].shape
    _, tile, f = h1.shape
    tps = cap // tile
    fh = f // 2
    rows = BT * tile
    fc = 512
    nc = f // fc
    alias = halves is not None

    def kernel(rng_ref, tl_ref, meta_ref, *refs):
        g_refs, refs = refs[:ng], refs[ng:]
        h1_ref, h3_ref, w1_hbm, w3_hbm, w2_hbm = refs[:5]
        refs = refs[5 + (3 if alias else 0):]
        dxd_refs, refs = refs[:ng], refs[ng:]
        (a_ref, dh1_ref, dh3_ref, w13v, w2v, gall, h1b, h3b, oall, hb, acc,
         wsem, gsem, isem, osem, hsem) = refs
        b0, b1 = rng_ref[at[0]], rng_ref[at[1]]
        half, me = meta_ref[0], meta_ref[1]
        c0 = half * (nc // 2)

        def src_tile(t):
            return lax.bitwise_xor(t // tps, me) * tps + lax.rem(t, tps)

        def tile_copies(b, slot, j):
            t = src_tile(tl_ref[b * BT + j])
            rs = pl.ds(j * tile, tile)
            return (pltpu.make_async_copy(h1_ref.at[t], h1b.at[slot, rs], isem.at[slot, 0, j]),
                    pltpu.make_async_copy(h3_ref.at[t], h3b.at[slot, rs], isem.at[slot, 1, j]))

        def fetch(b, slot):
            for j in range(BT):
                @pl.when(tl_ref[b * BT + j] >= 0)
                def _():
                    for c in tile_copies(b, slot, j):
                        c.start()

                @pl.when(tl_ref[b * BT + j] < 0)
                def _():
                    rs = pl.ds(j * tile, tile)
                    h1b[slot, rs] = jnp.zeros((tile, f), BF16)
                    h3b[slot, rs] = jnp.zeros((tile, f), BF16)

        def arrive(b, slot):
            for j in range(BT):
                @pl.when(tl_ref[b * BT + j] >= 0)
                def _():
                    for c in tile_copies(b, slot, j):
                        c.wait()

        def half_copies(b):
            rs = pl.ds(pl.multiple_of(b * rows, rows), rows)
            return [pltpu.make_async_copy(hb.at[q], r.at[rs], hsem.at[q])
                    for q, r in enumerate((a_ref, dh1_ref, dh3_ref))]

        gcopies = [pltpu.make_async_copy(g_refs[q], gall.at[pl.ds(q * cap, cap)], gsem.at[q]) for q in range(ng)]

        def wcopies(i, parts=(0, 1, 2)):
            c = lax.rem(c0 + i, nc)
            cs = pl.ds(pl.multiple_of(c * fc, fc), fc)
            return [pltpu.make_async_copy(w2_hbm.at[cs], w2v.at[cs], wsem.at[i, 0]) if q == 0 else
                    pltpu.make_async_copy((w1_hbm, w3_hbm)[q - 1].at[:, cs], w13v.at[c, :, pl.ds((q - 1) * fc, fc)],
                                          wsem.at[i, q])
                    for q in parts]

        for c in gcopies + wcopies(0, (0,)):
            c.start()

        @pl.when(b0 < b1)
        def _():
            fetch(b0, 0)

        for c in wcopies(0, (1, 2)):
            c.start()
        for i in range(1, nc):
            for c in wcopies(i):
                c.start()
        oall[...] = jnp.zeros(oall.shape, BF16)
        for c in gcopies:
            c.wait()

        def weights(b, i, part):
            @pl.when(b == b0)
            def _():
                for c in wcopies(i, part):
                    c.wait()

        @pl.loop(b0, b1)
        def _(b):
            slot = lax.rem(b - b0, 2)

            @pl.when(b + 1 < b1)
            def _():
                fetch(b + 1, 1 - slot)

            g = jnp.concatenate(
                [jnp.where(tl_ref[b * BT + j] >= 0,
                           gall[pl.ds(pl.multiple_of(jnp.maximum(tl_ref[b * BT + j] - first * tps, 0) * tile, tile), tile)],
                           jnp.zeros((tile, d), BF16)) for j in range(BT)], axis=0)
            arrive(b, slot)

            @pl.when(b > b0)
            def _():
                for c in half_copies(b - 1):
                    c.wait()

            def col(i):
                c = lax.rem(c0 + i, nc)
                return c, pl.ds(pl.multiple_of(c * fc, fc), fc)

            weights(b, 0, (0,))
            da = _dot_nt(g, w2v[col(0)[1], :])
            for i in range(nc):
                c, cs = col(i)
                weights(b, i, (1, 2))
                if i + 1 < nc:
                    weights(b, i + 1, (0,))
                nxt = _dot_nt(g, w2v[col(i + 1)[1], :]) if i + 1 < nc else None
                a, dh1, dh3 = _grads(da, h1b[slot, :, cs], h3b[slot, :, cs])
                if i < nc // 2:
                    hs = pl.ds(i * fc, fc)
                    hb[0, :, hs] = a
                    hb[1, :, hs] = dh1
                    hb[2, :, hs] = dh3
                y = _dot_nt(jnp.concatenate([dh1, dh3], axis=1), w13v[c])
                if i == 0:
                    acc[...] = y
                else:
                    acc[...] += y
                da = nxt
                if i == nc // 2 - 1:
                    for cp in half_copies(b):
                        cp.start()
            for j in range(BT):
                @pl.when(tl_ref[b * BT + j] >= 0)
                def _():
                    t = tl_ref[b * BT + j] - first * tps
                    oall[pl.ds(pl.multiple_of(t * tile, tile), tile)] = acc[pl.ds(j * tile, tile)].astype(BF16)

        @pl.when(b0 >= b1)
        def _():
            for i in range(nc):
                for c in wcopies(i):
                    c.wait()

        outs = [pltpu.make_async_copy(oall.at[pl.ds(q * cap, cap)], dxd_refs[q], osem.at[q]) for q in range(ng)]
        for c in outs:
            c.start()

        @pl.when(b0 < b1)
        def _():
            for c in half_copies(b1 - 1):
                c.wait()

        if alias:
            @pl.when(lax.rem(b1, 2) == 1)
            def _():
                hb[...] = jnp.zeros(hb.shape, BF16)
                for c in half_copies(b1):
                    c.start()
                for c in half_copies(b1):
                    c.wait()
        for c in outs:
            c.wait()

    hshape = jax.ShapeDtypeStruct((nblk * rows, fh), BF16)
    base = 3 + ng + 5
    return pl.pallas_call(
        kernel, in_specs=[SMEM] * 3 + [HBM] * (ng + 5 + (3 if alias else 0)), out_specs=[HBM] * (ng + 3),
        out_shape=[jax.ShapeDtypeStruct((cap, d), BF16)] * ng + [hshape] * 3,
        input_output_aliases={base + q: ng + q for q in range(3)} if alias else {},
        scratch_shapes=[pltpu.VMEM((nc, d, 2 * fc), BF16), pltpu.VMEM((f, d), BF16),
                        pltpu.VMEM((ng * cap, d), BF16), pltpu.VMEM((2, rows, f), BF16), pltpu.VMEM((2, rows, f), BF16),
                        pltpu.VMEM((ng * cap, d), BF16), pltpu.VMEM((3, rows, fh), BF16),
                        pltpu.VMEM((rows, d), F32),
                        pltpu.SemaphoreType.DMA((nc, 3)), pltpu.SemaphoreType.DMA((ng,)),
                        pltpu.SemaphoreType.DMA((2, 2, BT)), pltpu.SemaphoreType.DMA((ng,)),
                        pltpu.SemaphoreType.DMA((3,))],
        compiler_params=_params(), name="own_rows",
        cost_estimate=_cost(2 * 200 * ng * d * f * 3, 5e7),
    )(rng, tl, meta, *gs, h1, h3, w1, w3, w2, *(halves if alias else ()))


def _plan(occ, occo, meta, cut, tps, size):
    nt = occ.shape[0]

    def kernel(occ_ref, occo_ref, meta_ref, tl_ref, tlo_ref, bnd_ref):
        me = meta_ref[1]
        for li, (o_ref, t_ref) in enumerate(((occ_ref, tl_ref), (occo_ref, tlo_ref))):
            pos = jnp.int32(0)
            bnd_ref[li * 4] = pos
            for part, (lo, hi) in enumerate(((0, cut * tps), (cut * tps, nt))):
                def step(t, pos):
                    t_ref[pos] = t
                    return pos + o_ref[lax.bitwise_xor(t // tps, me) * tps + lax.rem(t, tps)]

                pos = lax.fori_loop(lo, hi, step, pos)
                end = ((pos + BT - 1) // BT) * BT

                def pad(i, c):
                    t_ref[i] = -1
                    return c

                lax.fori_loop(pos, end if part == 0 else end + BT, pad, 0)
                pos = end
                bnd_ref[li * 4 + 1 + part] = pos // BT
            bnd_ref[li * 4 + 3] = (pos // BT + 1) // 2

    return pl.pallas_call(
        kernel, in_specs=[SMEM] * 3, out_specs=[SMEM] * 3,
        out_shape=[jax.ShapeDtypeStruct((size,), I32), jax.ShapeDtypeStruct((size,), I32), jax.ShapeDtypeStruct((8,), I32)],
        name="plan", cost_estimate=_cost(1e6, 1e3))(occ, occo, meta)


def _dw(rng, tl, meta, first, gs, x, own, peer, sums, at, bt):
    ng = len(gs)
    cap, d = gs[0].shape
    _, tile, _ = x.shape
    tps = cap // tile
    fh = own[0].shape[1] if own else peer[0].shape[1] // 2
    rows = bt * tile
    fc = FC
    nc = fh // fc
    nadd = 3 if sums else 0
    mb = -(-ng * tps // bt) + (1 if own else 0)

    def kernel(rng_ref, tl_ref, meta_ref, *refs):
        g_refs, x_ref, refs = refs[:ng], refs[ng], refs[ng + 1:]
        s_refs, q_refs, o_refs = refs[:3], refs[3:3 + nadd], refs[3 + nadd:6 + nadd]
        (gall, xb, xt, gb, sv, p1, p3, p2, gsem, xsem, ssem, psem, osem) = refs[6 + nadd:]
        b0, b1 = rng_ref[at[0]], rng_ref[at[1]]
        half, me = meta_ref[0], meta_ref[1]

        def xcopy(b, j):
            t = tl_ref[b * bt + j]
            t = lax.bitwise_xor(t // tps, me) * tps + lax.rem(t, tps) if own else t - first * tps
            return pltpu.make_async_copy(x_ref.at[t], xb.at[b - b0, pl.ds(j * tile, tile)], xsem.at[b - b0, j])

        gcopies = [pltpu.make_async_copy(g_refs[q], gall.at[pl.ds(q * cap, cap)], gsem.at[q]) for q in range(ng)]

        def pcopies(c, slot):
            cs = pl.ds(pl.multiple_of(c * fc, fc), fc)
            views = ((p1, (slice(None), cs)), (p3, (slice(None), cs)), (p2, (cs, slice(None))))
            return [pltpu.make_async_copy(q.at[ix], p.at[slot], psem.at[slot, r])
                    for r, (q, (p, ix)) in enumerate(zip(q_refs, views))]

        def ocopies(c, slot):
            cs = pl.ds(pl.multiple_of(c * fc, fc), fc)
            views = ((p1, (slice(None), cs)), (p3, (slice(None), cs)), (p2, (cs, slice(None))))
            return [pltpu.make_async_copy(p.at[slot], o.at[ix], osem.at[slot, r])
                    for r, (o, (p, ix)) in enumerate(zip(o_refs, views))]

        def wcopies(c, slot):
            cs = pl.ds(pl.multiple_of(half * fh + c * fc, fc), fc)
            return [pltpu.make_async_copy(s.at[:, cs] if r < 2 else s.at[cs], sv.at[slot, r], ssem.at[slot, r])
                    for r, s in enumerate(s_refs)]

        def scopies(c, b, slot):
            rs = pl.ds(pl.multiple_of(b * rows, rows), rows)
            cs = pl.ds(pl.multiple_of(c * fc, fc), fc)
            return [pltpu.make_async_copy(s.at[rs, cs], sv.at[slot, r], ssem.at[slot, r]) for r, s in enumerate(s_refs)]

        for c in gcopies:
            c.start()

        @pl.loop(b0, b1)
        def _(b):
            for j in range(bt):
                @pl.when(tl_ref[b * bt + j] >= 0)
                def _():
                    xcopy(b, j).start()

                @pl.when(tl_ref[b * bt + j] < 0)
                def _():
                    xb[b - b0, pl.ds(j * tile, tile)] = jnp.zeros((tile, d), BF16)

        if peer:
            for cp in wcopies(0, 0):
                cp.start()
        if sums:
            for cp in pcopies(0, 0):
                cp.start()
        if own:
            @pl.when(b0 < b1)
            def _():
                for cp in scopies(0, b0, 0):
                    cp.start()
        for c in gcopies:
            c.wait()

        @pl.loop(b0, b1)
        def _(b):
            for j in range(bt):
                @pl.when(tl_ref[b * bt + j] >= 0)
                def _():
                    xcopy(b, j).wait()
                    t = tl_ref[b * bt + j] - first * tps
                    gb[b - b0, pl.ds(j * tile, tile)] = gall[pl.ds(pl.multiple_of(t * tile, tile), tile)]

                @pl.when(tl_ref[b * bt + j] < 0)
                def _():
                    gb[b - b0, pl.ds(j * tile, tile)] = jnp.zeros((tile, d), BF16)
            xt[b - b0] = xb[b - b0].T

        @pl.loop(0, nc)
        def _(c):
            ps = lax.rem(c, 2)
            if peer:
                @pl.when(c + 1 < nc)
                def _():
                    for cp in wcopies(c + 1, 1 - ps):
                        cp.start()

                for cp in wcopies(c, ps):
                    cp.wait()

            if sums:
                @pl.when(c + 1 < nc)
                def _():
                    @pl.when(c >= 1)
                    def _():
                        for cp in ocopies(c - 1, 1 - ps):
                            cp.wait()

                    for cp in pcopies(c + 1, 1 - ps):
                        cp.start()

                for cp in pcopies(c, ps):
                    cp.wait()
            else:
                @pl.when(c >= 2)
                def _():
                    for cp in ocopies(c - 2, ps):
                        cp.wait()

                p1[ps] = jnp.zeros((d, fc), F32)
                p3[ps] = jnp.zeros((d, fc), F32)
                p2[ps] = jnp.zeros((fc, d), F32)

            @pl.loop(b0, b1)
            def _(b):
                i = b - b0
                if own:
                    slot = lax.rem(c * (b1 - b0) + i, 2)

                    @pl.when(b + 1 < b1)
                    def _():
                        for cp in scopies(c, b + 1, 1 - slot):
                            cp.start()

                    @pl.when((b + 1 == b1) & (c + 1 < nc))
                    def _():
                        for cp in scopies(c + 1, b0, 1 - slot):
                            cp.start()

                    for cp in scopies(c, b, slot):
                        cp.wait()
                    a, dh1, dh3 = sv[slot, 0], sv[slot, 1], sv[slot, 2]
                else:
                    h1 = _dot(xb[i], sv[ps, 0]).astype(BF16)
                    h3 = _dot(xb[i], sv[ps, 1]).astype(BF16)
                    da = _dot_nt(gb[i], sv[ps, 2])
                    a, dh1, dh3 = _grads(da, h1, h3)
                p1[ps] += _dot(xt[i], dh1)
                p3[ps] += _dot(xt[i], dh3)
                p2[ps] += _dot(a.T, gb[i])

            for cp in ocopies(c, ps):
                cp.start()

        for c in (nc - 2, nc - 1):
            for cp in ocopies(c, c % 2):
                cp.wait()

    srows = rows if own else d
    outs = [jax.ShapeDtypeStruct((d, fh), F32), jax.ShapeDtypeStruct((d, fh), F32), jax.ShapeDtypeStruct((fh, d), F32)]
    return pl.pallas_call(
        kernel, in_specs=[SMEM] * 3 + [HBM] * (ng + 4 + nadd), out_specs=[HBM] * 3, out_shape=outs,
        scratch_shapes=[pltpu.VMEM((ng * cap, d), BF16), pltpu.VMEM((mb, rows, d), BF16), pltpu.VMEM((mb, d, rows), BF16),
                        pltpu.VMEM((mb, rows, d), BF16), pltpu.VMEM((2, 3, srows, fc), BF16),
                        pltpu.VMEM((2, d, fc), F32), pltpu.VMEM((2, d, fc), F32), pltpu.VMEM((2, fc, d), F32),
                        pltpu.SemaphoreType.DMA((ng,)), pltpu.SemaphoreType.DMA((mb, bt)),
                        pltpu.SemaphoreType.DMA((2, 3)), pltpu.SemaphoreType.DMA((2, 3)), pltpu.SemaphoreType.DMA((2, 3))],
        compiler_params=_params(), name="own_dw" if own else "peer_dw",
        cost_estimate=_cost(2 * 200 * ng * d * fh * (3 if own else 6), 5e7),
    )(rng, tl, meta, *gs, x, *(own or peer), *(sums or ()))


def solution(mesh):
    ne = mesh.shape['expert']
    nd = mesh.shape['data']
    tok = P(('data', 'expert'), None)
    buf = P(('data', 'expert'), None, None)
    wsp = P('expert', None, None)
    zswap = [(i, nd - 1 - i) for i in range(nd)]
    ka = ne * 3 // 4
    groups = ((2, 4, 3, 5), (6, 7, 1, 0))

    def run(dy, gates, topk_idx, slot, yd, xd, h1, h3, w1, w3, w2):
        t, d = dy.shape
        cap = xd.shape[1] // ne
        f = w1.shape[2]
        nt = xd.shape[1] // TILE
        tps = cap // TILE
        me = lax.axis_index('expert').astype(I32)
        grp = lax.axis_index('data').astype(I32)
        meta = jnp.stack([grp, me])
        xor = lambda k: [(i, i ^ k) for i in range(ne)]
        swap = lambda v: lax.ppermute(v, 'data', zswap)

        x4 = xd.reshape(nt, TILE, d)
        x8 = xd.reshape(ne, cap, d)
        xk = [lax.dynamic_index_in_dim(x8, me ^ k, 0, keepdims=True) for k in range(ne)]
        xo = [swap(jnp.concatenate(xk[i:j], axis=0).reshape((j - i) * tps, TILE, d)) for i, j in ((0, ka), (ka, ne))]

        send = [None] * ne
        for ks in groups:
            for k, v in zip(ks, _scatter_rows(topk_idx.reshape(1, t), slot.reshape(1, t), gates, dy, meta, ks, cap)):
                send[k] = v
        dyd = [send[0]]
        for k in range(1, ne):
            dyd.append(lax.ppermute(send[k], 'expert', xor(k)))
        dyo = []
        for k in range(ne):
            dyo.append(swap(dyd[k]))

        occ = jnp.any(x4 != 0, axis=(1, 2)).astype(I32)
        occo = swap(occ)
        nblk = -(-ka * tps // BT) + -(-(ne - ka) * tps // BT) + 1
        tl, tlo, bnd = _plan(occ, occo, meta, ka, tps, (nblk + 1) * BT)

        h14, h34 = h1.reshape(nt, TILE, f), h3.reshape(nt, TILE, f)
        wts = (w1[0], w3[0], w2[0])
        *da, ha, hd1, hd3 = _own_rows(bnd, tl, meta, 0, dyd[:ka], h14, h34, *wts, None, nblk, (0, 1))
        back = [da[0]]
        for k in range(1, ka):
            back.append(lax.ppermute(da[k], 'expert', xor(k)))
        *db, ha, hd1, hd3 = _own_rows(bnd, tl, meta, ka, dyd[ka:], h14, h34, *wts, (ha, hd1, hd3), nblk, (1, 2))
        for k in range(ka, ne):
            back.append(lax.ppermute(db[k - ka], 'expert', xor(k)))
        sums = _dw(bnd, tl, meta, 0, dyd, x4, (ha, hd1, hd3), None, None, (0, 3), 2 * BT)
        dg = jnp.einsum('tkd,td->tk', yd, dy, preferred_element_type=F32)
        cpos = jnp.where(slot >= 0, (topk_idx ^ me) * cap + slot, -1)
        dx = _gather_rows(cpos, back)
        sums = _dw(bnd, tlo, meta, 0, dyo[:ka], xo[0], None, wts, sums, (4, 5), BT)
        sums = _dw(bnd, tlo, meta, ka, dyo[ka:], xo[1], None, wts, sums, (5, 6), BT)
        dw1, dw3, dw2 = sums
        return dx, dg, dw1[None], dw3[None], dw2[None]


    return jax.shard_map(run, mesh=mesh,
                         in_specs=(tok, tok, tok, tok, buf, buf, buf, buf, wsp, wsp, wsp),
                         out_specs=(tok, tok, P('expert', None, 'data'), P('expert', None, 'data'), P('expert', 'data', None)),
                         check_vma=False)
```

```python
import jax
import jax.numpy as jnp
from jax import lax
from jax.experimental import pallas as pl
from jax.experimental.pallas import tpu as pltpu
from jax.sharding import PartitionSpec as P


F32 = jnp.float32
BF16 = jnp.bfloat16
I32 = jnp.int32


TILE = 64
BT = 4
FC = 768
VMEM_LIMIT = 62 * 1024 * 1024

ANY = pl.BlockSpec(memory_space=pl.ANY)
HBM = pl.BlockSpec(memory_space=pltpu.HBM)
SMEM = pl.BlockSpec(memory_space=pltpu.SMEM)


def _params(**kw):
    return pltpu.CompilerParams(vmem_limit_bytes=VMEM_LIMIT, **kw)


def _cost(flops, nbytes):
    return pl.CostEstimate(flops=int(flops), bytes_accessed=int(nbytes), transcendentals=0)


def _dot(a, b):
    return jnp.dot(a, b, preferred_element_type=F32)


def _dot_nt(a, b):
    return lax.dot_general(a, b, (((1,), (1,)), ((), ())), preferred_element_type=F32)


def _grads(da, h1, h3):
    h1f = h1.astype(F32)
    h3f = h3.astype(F32)
    da = da.astype(BF16).astype(F32)
    s = jax.nn.sigmoid(h1f)
    silu = h1f * s
    a = (silu * h3f).astype(BF16)
    dh1 = ((da * h3f) * (s + silu * (1.0 - s))).astype(BF16)
    dh3 = (da * silu).astype(BF16)
    return a, dh1, dh3


def _scatter_rows(topk, slot, gates, dy, me, ks, cap):
    t, d = dy.shape
    k = len(ks)

    def kernel(meta_ref, e_ref, s_ref, g_ref, dy_ref, *refs):
        outs, v_ref, ob, sem = refs[:k], refs[k], refs[k + 1], refs[k + 2]
        v_ref[...] = (g_ref[...] * dy_ref[...].astype(F32)).astype(BF16)

        @pl.loop(0, k)
        def _(q):
            kq = sum(jnp.where(q == p, ks[p], 0) for p in range(k))
            pos = jnp.where(e_ref[...] == lax.bitwise_xor(kq, meta_ref[1]), s_ref[...], -1)
            row = lax.broadcasted_iota(I32, (cap, t), 0)
            oh = jnp.where(pos == row, 1.0, 0.0).astype(BF16)
            ob[q] = _dot(oh, v_ref[...]).astype(BF16)
            for p in range(k):
                @pl.when(q == p)
                def _():
                    pltpu.make_async_copy(ob.at[p], outs[p], sem.at[p]).start()

        for p in range(k):
            pltpu.make_async_copy(ob.at[p], outs[p], sem.at[p]).wait()

    vm = pl.BlockSpec(memory_space=pltpu.VMEM)
    return pl.pallas_call(
        kernel, in_specs=[SMEM] + [vm] * 4, out_specs=[HBM] * k,
        out_shape=[jax.ShapeDtypeStruct((cap, d), BF16)] * k,
        scratch_shapes=[pltpu.VMEM((t, d), BF16), pltpu.VMEM((k, cap, d), BF16), pltpu.SemaphoreType.DMA((k,))],
        compiler_params=_params(), name="scatter_rows",
        cost_estimate=_cost(2 * k * cap * t * d, 2 * k * cap * d * 2),
    )(me, topk, slot, gates, dy)


def _gather_rows(pos, parts):
    t = pos.shape[0]
    k = len(parts)
    r, d = parts[0].shape
    tb = 512

    def kernel(pos_ref, *refs):
        ins, o_ref, src, sem = refs[:k], refs[k], refs[k + 1], refs[k + 2]

        @pl.when(pl.program_id(0) == 0)
        def _():
            for q in range(k):
                pltpu.make_async_copy(ins[q], src.at[pl.ds(q * r, r)], sem.at[q]).start()
            for q in range(k):
                pltpu.make_async_copy(ins[q], src.at[pl.ds(q * r, r)], sem.at[q]).wait()

        col = lax.broadcasted_iota(I32, (tb, k * r), 1)
        oh = jnp.where(pos_ref[...] == col, 1.0, 0.0).astype(BF16)
        o_ref[...] = _dot(oh, src[...]).astype(BF16)

    return pl.pallas_call(
        kernel, grid=(t // tb,),
        in_specs=[pl.BlockSpec((tb, 1), lambda i: (i, 0))] + [HBM] * k,
        out_specs=pl.BlockSpec((tb, d), lambda i: (i, 0)),
        out_shape=jax.ShapeDtypeStruct((t, d), BF16),
        scratch_shapes=[pltpu.VMEM((k * r, d), BF16), pltpu.SemaphoreType.DMA((k,))],
        compiler_params=_params(), name="gather_rows",
        cost_estimate=_cost(2 * k * r * t * d, 2 * k * r * d * 2),
    )(pos, *parts)


def _own_rows(rng, tl, meta, first, gs, h1, h3, w1, w3, w2, halves, nblk, at):
    ng = len(gs)
    cap, d = gs[0].shape
    _, tile, f = h1.shape
    tps = cap // tile
    fh = f // 2
    rows = BT * tile
    fc = 512
    nc = f // fc
    alias = halves is not None

    def kernel(rng_ref, tl_ref, meta_ref, *refs):
        g_refs, refs = refs[:ng], refs[ng:]
        h1_ref, h3_ref, w1_hbm, w3_hbm, w2_hbm = refs[:5]
        refs = refs[5 + (3 if alias else 0):]
        dxd_refs, refs = refs[:ng], refs[ng:]
        (a_ref, dh1_ref, dh3_ref, w13v, w2v, gall, h1b, h3b, oall, hb, acc,
         wsem, gsem, isem, osem, hsem) = refs
        b0, b1 = rng_ref[at[0]], rng_ref[at[1]]
        half, me = meta_ref[0], meta_ref[1]
        c0 = half * (nc // 2)

        def src_tile(t):
            return lax.bitwise_xor(t // tps, me) * tps + lax.rem(t, tps)

        def tile_copies(b, slot, j):
            t = src_tile(tl_ref[b * BT + j])
            rs = pl.ds(j * tile, tile)
            return (pltpu.make_async_copy(h1_ref.at[t], h1b.at[slot, rs], isem.at[slot, 0, j]),
                    pltpu.make_async_copy(h3_ref.at[t], h3b.at[slot, rs], isem.at[slot, 1, j]))

        def fetch(b, slot):
            for j in range(BT):
                @pl.when(tl_ref[b * BT + j] >= 0)
                def _():
                    for c in tile_copies(b, slot, j):
                        c.start()

                @pl.when(tl_ref[b * BT + j] < 0)
                def _():
                    rs = pl.ds(j * tile, tile)
                    h1b[slot, rs] = jnp.zeros((tile, f), BF16)
                    h3b[slot, rs] = jnp.zeros((tile, f), BF16)

        def arrive(b, slot):
            for j in range(BT):
                @pl.when(tl_ref[b * BT + j] >= 0)
                def _():
                    for c in tile_copies(b, slot, j):
                        c.wait()

        def half_copies(b):
            rs = pl.ds(pl.multiple_of(b * rows, rows), rows)
            return [pltpu.make_async_copy(hb.at[q], r.at[rs], hsem.at[q])
                    for q, r in enumerate((a_ref, dh1_ref, dh3_ref))]

        gcopies = [pltpu.make_async_copy(g_refs[q], gall.at[pl.ds(q * cap, cap)], gsem.at[q]) for q in range(ng)]

        def wcopies(i, parts=(0, 1, 2)):
            c = lax.rem(c0 + i, nc)
            cs = pl.ds(pl.multiple_of(c * fc, fc), fc)
            return [pltpu.make_async_copy(w2_hbm.at[cs], w2v.at[cs], wsem.at[i, 0]) if q == 0 else
                    pltpu.make_async_copy((w1_hbm, w3_hbm)[q - 1].at[:, cs], w13v.at[c, :, pl.ds((q - 1) * fc, fc)],
                                          wsem.at[i, q])
                    for q in parts]

        for c in gcopies + wcopies(0, (0,)):
            c.start()

        @pl.when(b0 < b1)
        def _():
            fetch(b0, 0)

        for c in wcopies(0, (1, 2)):
            c.start()
        for i in range(1, nc):
            for c in wcopies(i):
                c.start()
        oall[...] = jnp.zeros(oall.shape, BF16)
        for c in gcopies:
            c.wait()

        def weights(b, i, part):
            @pl.when(b == b0)
            def _():
                for c in wcopies(i, part):
                    c.wait()

        @pl.loop(b0, b1)
        def _(b):
            slot = lax.rem(b - b0, 2)

            @pl.when(b + 1 < b1)
            def _():
                fetch(b + 1, 1 - slot)

            g = jnp.concatenate(
                [jnp.where(tl_ref[b * BT + j] >= 0,
                           gall[pl.ds(pl.multiple_of(jnp.maximum(tl_ref[b * BT + j] - first * tps, 0) * tile, tile), tile)],
                           jnp.zeros((tile, d), BF16)) for j in range(BT)], axis=0)
            arrive(b, slot)

            @pl.when(b > b0)
            def _():
                for c in half_copies(b - 1):
                    c.wait()

            def col(i):
                c = lax.rem(c0 + i, nc)
                return c, pl.ds(pl.multiple_of(c * fc, fc), fc)

            weights(b, 0, (0,))
            da = _dot_nt(g, w2v[col(0)[1], :])
            for i in range(nc):
                c, cs = col(i)
                weights(b, i, (1, 2))
                if i + 1 < nc:
                    weights(b, i + 1, (0,))
                nxt = _dot_nt(g, w2v[col(i + 1)[1], :]) if i + 1 < nc else None
                a, dh1, dh3 = _grads(da, h1b[slot, :, cs], h3b[slot, :, cs])
                if i < nc // 2:
                    hs = pl.ds(i * fc, fc)
                    hb[0, :, hs] = a
                    hb[1, :, hs] = dh1
                    hb[2, :, hs] = dh3
                y = _dot_nt(jnp.concatenate([dh1, dh3], axis=1), w13v[c])
                if i == 0:
                    acc[...] = y
                else:
                    acc[...] += y
                da = nxt
                if i == nc // 2 - 1:
                    for cp in half_copies(b):
                        cp.start()
            for j in range(BT):
                @pl.when(tl_ref[b * BT + j] >= 0)
                def _():
                    t = tl_ref[b * BT + j] - first * tps
                    oall[pl.ds(pl.multiple_of(t * tile, tile), tile)] = acc[pl.ds(j * tile, tile)].astype(BF16)

        @pl.when(b0 >= b1)
        def _():
            for i in range(nc):
                for c in wcopies(i):
                    c.wait()

        outs = [pltpu.make_async_copy(oall.at[pl.ds(q * cap, cap)], dxd_refs[q], osem.at[q]) for q in range(ng)]
        for c in outs:
            c.start()

        @pl.when(b0 < b1)
        def _():
            for c in half_copies(b1 - 1):
                c.wait()

        if alias:
            @pl.when(lax.rem(b1, 2) == 1)
            def _():
                hb[...] = jnp.zeros(hb.shape, BF16)
                for c in half_copies(b1):
                    c.start()
                for c in half_copies(b1):
                    c.wait()
        for c in outs:
            c.wait()

    hshape = jax.ShapeDtypeStruct((nblk * rows, fh), BF16)
    base = 3 + ng + 5
    return pl.pallas_call(
        kernel, in_specs=[SMEM] * 3 + [HBM] * (ng + 5 + (3 if alias else 0)), out_specs=[HBM] * (ng + 3),
        out_shape=[jax.ShapeDtypeStruct((cap, d), BF16)] * ng + [hshape] * 3,
        input_output_aliases={base + q: ng + q for q in range(3)} if alias else {},
        scratch_shapes=[pltpu.VMEM((nc, d, 2 * fc), BF16), pltpu.VMEM((f, d), BF16),
                        pltpu.VMEM((ng * cap, d), BF16), pltpu.VMEM((2, rows, f), BF16), pltpu.VMEM((2, rows, f), BF16),
                        pltpu.VMEM((ng * cap, d), BF16), pltpu.VMEM((3, rows, fh), BF16),
                        pltpu.VMEM((rows, d), F32),
                        pltpu.SemaphoreType.DMA((nc, 3)), pltpu.SemaphoreType.DMA((ng,)),
                        pltpu.SemaphoreType.DMA((2, 2, BT)), pltpu.SemaphoreType.DMA((ng,)),
                        pltpu.SemaphoreType.DMA((3,))],
        compiler_params=_params(), name="own_rows",
        cost_estimate=_cost(2 * 200 * ng * d * f * 3, 5e7),
    )(rng, tl, meta, *gs, h1, h3, w1, w3, w2, *(halves if alias else ()))


def _plan(occ, meta, cut, tps, size):
    nt = occ.shape[0]

    def kernel(occ_ref, meta_ref, tl_ref, bnd_ref):
        me = meta_ref[1]
        pos = jnp.int32(0)
        bnd_ref[0] = pos
        for part, (lo, hi) in enumerate(((0, cut * tps), (cut * tps, nt))):
            def step(t, pos):
                tl_ref[pos] = t
                return pos + occ_ref[lax.bitwise_xor(t // tps, me) * tps + lax.rem(t, tps)]

            pos = lax.fori_loop(lo, hi, step, pos)
            end = ((pos + BT - 1) // BT) * BT

            def pad(i, c):
                tl_ref[i] = -1
                return c

            lax.fori_loop(pos, end if part == 0 else end + BT, pad, 0)
            pos = end
            bnd_ref[1 + part] = pos // BT
        bnd_ref[3] = (pos // BT + 1) // 2

    return pl.pallas_call(
        kernel, in_specs=[SMEM] * 2, out_specs=[SMEM] * 2,
        out_shape=[jax.ShapeDtypeStruct((size,), I32), jax.ShapeDtypeStruct((8,), I32)],
        name="plan", cost_estimate=_cost(1e6, 1e3))(occ, meta)


def _dw(rng, tl, meta, first, gs, x, own, peer, sums, at, bt):
    ng = len(gs)
    cap, d = gs[0].shape
    _, tile, _ = x.shape
    tps = cap // tile
    fh = own[0].shape[1] if own else peer[0].shape[1] // 2
    rows = bt * tile
    fc = FC
    nc = fh // fc
    nadd = 3 if sums else 0
    mb = -(-ng * tps // bt) + (1 if own else 0)

    def kernel(rng_ref, tl_ref, meta_ref, *refs):
        g_refs, x_ref, refs = refs[:ng], refs[ng], refs[ng + 1:]
        s_refs, q_refs, o_refs = refs[:3], refs[3:3 + nadd], refs[3 + nadd:6 + nadd]
        (gall, xb, xt, gb, sv, p1, p3, p2, gsem, xsem, ssem, psem, osem) = refs[6 + nadd:]
        b0, b1 = rng_ref[at[0]], rng_ref[at[1]]
        half, me = meta_ref[0], meta_ref[1]

        def xcopy(b, j):
            t = tl_ref[b * bt + j]
            t = lax.bitwise_xor(t // tps, me) * tps + lax.rem(t, tps)
            return pltpu.make_async_copy(x_ref.at[t], xb.at[b - b0, pl.ds(j * tile, tile)], xsem.at[b - b0, j])

        gcopies = [pltpu.make_async_copy(g_refs[q], gall.at[pl.ds(q * cap, cap)], gsem.at[q]) for q in range(ng)]

        def pcopies(c, slot):
            cs = pl.ds(pl.multiple_of(c * fc, fc), fc)
            views = ((p1, (slice(None), cs)), (p3, (slice(None), cs)), (p2, (cs, slice(None))))
            return [pltpu.make_async_copy(q.at[ix], p.at[slot], psem.at[slot, r])
                    for r, (q, (p, ix)) in enumerate(zip(q_refs, views))]

        def ocopies(c, slot):
            cs = pl.ds(pl.multiple_of(c * fc, fc), fc)
            views = ((p1, (slice(None), cs)), (p3, (slice(None), cs)), (p2, (cs, slice(None))))
            return [pltpu.make_async_copy(p.at[slot], o.at[ix], osem.at[slot, r])
                    for r, (o, (p, ix)) in enumerate(zip(o_refs, views))]

        def wcopies(c, slot):
            cs = pl.ds(pl.multiple_of(half * fh + c * fc, fc), fc)
            return [pltpu.make_async_copy(s.at[:, cs] if r < 2 else s.at[cs], sv.at[slot, r], ssem.at[slot, r])
                    for r, s in enumerate(s_refs)]

        def scopies(c, b, slot):
            rs = pl.ds(pl.multiple_of(b * rows, rows), rows)
            cs = pl.ds(pl.multiple_of(c * fc, fc), fc)
            return [pltpu.make_async_copy(s.at[rs, cs], sv.at[slot, r], ssem.at[slot, r]) for r, s in enumerate(s_refs)]

        for c in gcopies:
            c.start()

        @pl.loop(b0, b1)
        def _(b):
            for j in range(bt):
                @pl.when(tl_ref[b * bt + j] >= 0)
                def _():
                    xcopy(b, j).start()

                @pl.when(tl_ref[b * bt + j] < 0)
                def _():
                    xb[b - b0, pl.ds(j * tile, tile)] = jnp.zeros((tile, d), BF16)

        if peer:
            for cp in wcopies(0, 0):
                cp.start()
        if sums:
            for cp in pcopies(0, 0):
                cp.start()
        if own:
            @pl.when(b0 < b1)
            def _():
                for cp in scopies(0, b0, 0):
                    cp.start()
        for c in gcopies:
            c.wait()

        @pl.loop(b0, b1)
        def _(b):
            for j in range(bt):
                @pl.when(tl_ref[b * bt + j] >= 0)
                def _():
                    xcopy(b, j).wait()
                    t = tl_ref[b * bt + j] - first * tps
                    gb[b - b0, pl.ds(j * tile, tile)] = gall[pl.ds(pl.multiple_of(t * tile, tile), tile)]

                @pl.when(tl_ref[b * bt + j] < 0)
                def _():
                    gb[b - b0, pl.ds(j * tile, tile)] = jnp.zeros((tile, d), BF16)
            xt[b - b0] = xb[b - b0].T

        @pl.loop(0, nc)
        def _(c):
            ps = lax.rem(c, 2)
            if peer:
                @pl.when(c + 1 < nc)
                def _():
                    for cp in wcopies(c + 1, 1 - ps):
                        cp.start()

                for cp in wcopies(c, ps):
                    cp.wait()

            if sums:
                @pl.when(c + 1 < nc)
                def _():
                    @pl.when(c >= 1)
                    def _():
                        for cp in ocopies(c - 1, 1 - ps):
                            cp.wait()

                    for cp in pcopies(c + 1, 1 - ps):
                        cp.start()

                for cp in pcopies(c, ps):
                    cp.wait()
            else:
                @pl.when(c >= 2)
                def _():
                    for cp in ocopies(c - 2, ps):
                        cp.wait()

                p1[ps] = jnp.zeros((d, fc), F32)
                p3[ps] = jnp.zeros((d, fc), F32)
                p2[ps] = jnp.zeros((fc, d), F32)

            @pl.loop(b0, b1)
            def _(b):
                i = b - b0
                if own:
                    slot = lax.rem(c * (b1 - b0) + i, 2)

                    @pl.when(b + 1 < b1)
                    def _():
                        for cp in scopies(c, b + 1, 1 - slot):
                            cp.start()

                    @pl.when((b + 1 == b1) & (c + 1 < nc))
                    def _():
                        for cp in scopies(c + 1, b0, 1 - slot):
                            cp.start()

                    for cp in scopies(c, b, slot):
                        cp.wait()
                    a, dh1, dh3 = sv[slot, 0], sv[slot, 1], sv[slot, 2]
                else:
                    h1 = _dot(xb[i], sv[ps, 0]).astype(BF16)
                    h3 = _dot(xb[i], sv[ps, 1]).astype(BF16)
                    da = _dot_nt(gb[i], sv[ps, 2])
                    a, dh1, dh3 = _grads(da, h1, h3)
                p1[ps] += _dot(xt[i], dh1)
                p3[ps] += _dot(xt[i], dh3)
                p2[ps] += _dot(a.T, gb[i])

            for cp in ocopies(c, ps):
                cp.start()

        for c in (nc - 2, nc - 1):
            for cp in ocopies(c, c % 2):
                cp.wait()

    srows = rows if own else d
    outs = [jax.ShapeDtypeStruct((d, fh), F32), jax.ShapeDtypeStruct((d, fh), F32), jax.ShapeDtypeStruct((fh, d), F32)]
    return pl.pallas_call(
        kernel, in_specs=[SMEM] * 3 + [HBM] * (ng + 4 + nadd), out_specs=[HBM] * 3, out_shape=outs,
        scratch_shapes=[pltpu.VMEM((ng * cap, d), BF16), pltpu.VMEM((mb, rows, d), BF16), pltpu.VMEM((mb, d, rows), BF16),
                        pltpu.VMEM((mb, rows, d), BF16), pltpu.VMEM((2, 3, srows, fc), BF16),
                        pltpu.VMEM((2, d, fc), F32), pltpu.VMEM((2, d, fc), F32), pltpu.VMEM((2, fc, d), F32),
                        pltpu.SemaphoreType.DMA((ng,)), pltpu.SemaphoreType.DMA((mb, bt)),
                        pltpu.SemaphoreType.DMA((2, 3)), pltpu.SemaphoreType.DMA((2, 3)), pltpu.SemaphoreType.DMA((2, 3))],
        compiler_params=_params(), name="own_dw" if own else "peer_dw",
        cost_estimate=_cost(2 * 200 * ng * d * fh * (3 if own else 6), 5e7),
    )(rng, tl, meta, *gs, x, *(own or peer), *(sums or ()))


def solution(mesh):
    ne = mesh.shape['expert']
    nd = mesh.shape['data']
    tok = P(('data', 'expert'), None)
    buf = P(('data', 'expert'), None, None)
    wsp = P('expert', None, None)
    zswap = [(i, nd - 1 - i) for i in range(nd)]
    ka = ne * 3 // 4
    groups = ((2, 4, 3, 5), (6, 7, 1, 0))

    def run(dy, gates, topk_idx, slot, yd, xd, h1, h3, w1, w3, w2):
        t, d = dy.shape
        cap = xd.shape[1] // ne
        f = w1.shape[2]
        nt = xd.shape[1] // TILE
        tps = cap // TILE
        me = lax.axis_index('expert').astype(I32)
        grp = lax.axis_index('data').astype(I32)
        meta = jnp.stack([grp, me])
        xor = lambda k: [(i, i ^ k) for i in range(ne)]
        swap = lambda v: lax.ppermute(v, 'data', zswap)

        x4 = xd.reshape(nt, TILE, d)
        xo = swap(x4)

        send = [None] * ne
        for ks in groups:
            for k, v in zip(ks, _scatter_rows(topk_idx.reshape(1, t), slot.reshape(1, t), gates, dy, meta, ks, cap)):
                send[k] = v
        dyd = [send[0]]
        for k in range(1, ne):
            dyd.append(lax.ppermute(send[k], 'expert', xor(k)))
        dyo = []
        for k in range(ne):
            dyo.append(swap(dyd[k]))

        occ = jnp.any(x4 != 0, axis=(1, 2)).astype(I32)
        occo = swap(occ)
        nblk = -(-ka * tps // BT) + -(-(ne - ka) * tps // BT) + 1
        tl, bnd = _plan(occ, meta, ka, tps, (nblk + 1) * BT)
        tlo, bndo = _plan(occo, meta, ka, tps, (nblk + 1) * BT)

        h14, h34 = h1.reshape(nt, TILE, f), h3.reshape(nt, TILE, f)
        wts = (w1[0], w3[0], w2[0])
        *da, ha, hd1, hd3 = _own_rows(bnd, tl, meta, 0, dyd[:ka], h14, h34, *wts, None, nblk, (0, 1))
        back = [da[0]]
        for k in range(1, ka):
            back.append(lax.ppermute(da[k], 'expert', xor(k)))
        *db, ha, hd1, hd3 = _own_rows(bnd, tl, meta, ka, dyd[ka:], h14, h34, *wts, (ha, hd1, hd3), nblk, (1, 2))
        for k in range(ka, ne):
            back.append(lax.ppermute(db[k - ka], 'expert', xor(k)))
        sums = _dw(bnd, tl, meta, 0, dyd, x4, (ha, hd1, hd3), None, None, (0, 3), 2 * BT)
        dg = jnp.einsum('tkd,td->tk', yd, dy, preferred_element_type=F32)
        cpos = jnp.where(slot >= 0, (topk_idx ^ me) * cap + slot, -1)
        dx = _gather_rows(cpos, back)
        sums = _dw(bndo, tlo, meta, 0, dyo[:ka], xo, None, wts, sums, (0, 1), BT)
        sums = _dw(bndo, tlo, meta, ka, dyo[ka:], xo, None, wts, sums, (1, 2), BT)
        dw1, dw3, dw2 = sums
        return dx, dg, dw1[None], dw3[None], dw2[None]


    return jax.shard_map(run, mesh=mesh,
                         in_specs=(tok, tok, tok, tok, buf, buf, buf, buf, wsp, wsp, wsp),
                         out_specs=(tok, tok, P('expert', None, 'data'), P('expert', None, 'data'), P('expert', 'data', None)),
                         check_vma=False)
```

```python
import jax
import jax.numpy as jnp
from jax import lax
from jax.experimental import pallas as pl
from jax.experimental.pallas import tpu as pltpu
from jax.sharding import PartitionSpec as P


F32 = jnp.float32
BF16 = jnp.bfloat16
I32 = jnp.int32


TILE = 64
BT = 4
FC = 768
VMEM_LIMIT = 62 * 1024 * 1024

ANY = pl.BlockSpec(memory_space=pl.ANY)
HBM = pl.BlockSpec(memory_space=pltpu.HBM)
SMEM = pl.BlockSpec(memory_space=pltpu.SMEM)


def _params(**kw):
    return pltpu.CompilerParams(vmem_limit_bytes=VMEM_LIMIT, **kw)


def _cost(flops, nbytes):
    return pl.CostEstimate(flops=int(flops), bytes_accessed=int(nbytes), transcendentals=0)


def _dot(a, b):
    return jnp.dot(a, b, preferred_element_type=F32)


def _dot_nt(a, b):
    return lax.dot_general(a, b, (((1,), (1,)), ((), ())), preferred_element_type=F32)


def _grads(da, h1, h3):
    h1f = h1.astype(F32)
    h3f = h3.astype(F32)
    da = da.astype(BF16).astype(F32)
    s = jax.nn.sigmoid(h1f)
    silu = h1f * s
    a = (silu * h3f).astype(BF16)
    dh1 = ((da * h3f) * (s + silu * (1.0 - s))).astype(BF16)
    dh3 = (da * silu).astype(BF16)
    return a, dh1, dh3


def _scatter_rows(topk, slot, gates, dy, me, ks, cap):
    t, d = dy.shape
    k = len(ks)

    def kernel(meta_ref, e_ref, s_ref, g_ref, dy_ref, *refs):
        outs, v_ref, ob, sem = refs[:k], refs[k], refs[k + 1], refs[k + 2]
        col = jnp.broadcast_to(g_ref[...], (128, t)).T
        for c in range(0, d, 128):
            v_ref[:, c:c + 128] = (col * dy_ref[:, c:c + 128].astype(F32)).astype(BF16)

        @pl.loop(0, k)
        def _(q):
            kq = sum(jnp.where(q == p, ks[p], 0) for p in range(k))
            pos = jnp.where(e_ref[...] == lax.bitwise_xor(kq, meta_ref[1]), s_ref[...], -1)
            row = lax.broadcasted_iota(I32, (cap, t), 0)
            oh = jnp.where(pos == row, 1.0, 0.0).astype(BF16)
            ob[q] = _dot(oh, v_ref[...]).astype(BF16)
            for p in range(k):
                @pl.when(q == p)
                def _():
                    pltpu.make_async_copy(ob.at[p], outs[p], sem.at[p]).start()

        for p in range(k):
            pltpu.make_async_copy(ob.at[p], outs[p], sem.at[p]).wait()

    vm = pl.BlockSpec(memory_space=pltpu.VMEM)
    return pl.pallas_call(
        kernel, in_specs=[SMEM] + [vm] * 4, out_specs=[HBM] * k,
        out_shape=[jax.ShapeDtypeStruct((cap, d), BF16)] * k,
        scratch_shapes=[pltpu.VMEM((t, d), BF16), pltpu.VMEM((k, cap, d), BF16), pltpu.SemaphoreType.DMA((k,))],
        compiler_params=_params(), name="scatter_rows",
        cost_estimate=_cost(2 * k * cap * t * d, 2 * k * cap * d * 2),
    )(me, topk, slot, gates, dy)


def _gather_rows(pos, parts):
    t = pos.shape[0]
    k = len(parts)
    r, d = parts[0].shape
    tb = 512

    def kernel(pos_ref, *refs):
        ins, o_ref, src, sem = refs[:k], refs[k], refs[k + 1], refs[k + 2]

        @pl.when(pl.program_id(0) == 0)
        def _():
            for q in range(k):
                pltpu.make_async_copy(ins[q], src.at[pl.ds(q * r, r)], sem.at[q]).start()
            for q in range(k):
                pltpu.make_async_copy(ins[q], src.at[pl.ds(q * r, r)], sem.at[q]).wait()

        col = lax.broadcasted_iota(I32, (tb, k * r), 1)
        oh = jnp.where(pos_ref[...] == col, 1.0, 0.0).astype(BF16)
        o_ref[...] = _dot(oh, src[...]).astype(BF16)

    return pl.pallas_call(
        kernel, grid=(t // tb,),
        in_specs=[pl.BlockSpec((tb, 1), lambda i: (i, 0))] + [HBM] * k,
        out_specs=pl.BlockSpec((tb, d), lambda i: (i, 0)),
        out_shape=jax.ShapeDtypeStruct((t, d), BF16),
        scratch_shapes=[pltpu.VMEM((k * r, d), BF16), pltpu.SemaphoreType.DMA((k,))],
        compiler_params=_params(), name="gather_rows",
        cost_estimate=_cost(2 * k * r * t * d, 2 * k * r * d * 2),
    )(pos, *parts)


def _own_rows(rng, tl, meta, first, gs, h1, h3, w1, w3, w2, halves, nblk, at):
    ng = len(gs)
    cap, d = gs[0].shape
    _, tile, f = h1.shape
    tps = cap // tile
    fh = f // 2
    rows = BT * tile
    fc = 512
    nc = f // fc
    alias = halves is not None

    def kernel(rng_ref, tl_ref, meta_ref, *refs):
        g_refs, refs = refs[:ng], refs[ng:]
        h1_ref, h3_ref, w1_hbm, w3_hbm, w2_hbm = refs[:5]
        refs = refs[5 + (3 if alias else 0):]
        dxd_refs, refs = refs[:ng], refs[ng:]
        (a_ref, dh1_ref, dh3_ref, w13v, w2v, gall, h1b, h3b, oall, hb, acc,
         wsem, gsem, isem, osem, hsem) = refs
        b0, b1 = rng_ref[at[0]], rng_ref[at[1]]
        half, me = meta_ref[0], meta_ref[1]
        c0 = half * (nc // 2)

        def src_tile(t):
            return lax.bitwise_xor(t // tps, me) * tps + lax.rem(t, tps)

        def tile_copies(b, slot, j):
            t = src_tile(tl_ref[b * BT + j])
            rs = pl.ds(j * tile, tile)
            return (pltpu.make_async_copy(h1_ref.at[t], h1b.at[slot, rs], isem.at[slot, 0, j]),
                    pltpu.make_async_copy(h3_ref.at[t], h3b.at[slot, rs], isem.at[slot, 1, j]))

        def fetch(b, slot):
            for j in range(BT):
                @pl.when(tl_ref[b * BT + j] >= 0)
                def _():
                    for c in tile_copies(b, slot, j):
                        c.start()

                @pl.when(tl_ref[b * BT + j] < 0)
                def _():
                    rs = pl.ds(j * tile, tile)
                    h1b[slot, rs] = jnp.zeros((tile, f), BF16)
                    h3b[slot, rs] = jnp.zeros((tile, f), BF16)

        def arrive(b, slot):
            for j in range(BT):
                @pl.when(tl_ref[b * BT + j] >= 0)
                def _():
                    for c in tile_copies(b, slot, j):
                        c.wait()

        def half_copies(b):
            rs = pl.ds(pl.multiple_of(b * rows, rows), rows)
            return [pltpu.make_async_copy(hb.at[q], r.at[rs], hsem.at[q])
                    for q, r in enumerate((a_ref, dh1_ref, dh3_ref))]

        gcopies = [pltpu.make_async_copy(g_refs[q], gall.at[pl.ds(q * cap, cap)], gsem.at[q]) for q in range(ng)]

        def wcopies(i, parts=(0, 1, 2)):
            c = lax.rem(c0 + i, nc)
            cs = pl.ds(pl.multiple_of(c * fc, fc), fc)
            return [pltpu.make_async_copy(w2_hbm.at[cs], w2v.at[cs], wsem.at[i, 0]) if q == 0 else
                    pltpu.make_async_copy((w1_hbm, w3_hbm)[q - 1].at[:, cs], w13v.at[c, :, pl.ds((q - 1) * fc, fc)],
                                          wsem.at[i, q])
                    for q in parts]

        for c in gcopies + wcopies(0, (0,)):
            c.start()

        @pl.when(b0 < b1)
        def _():
            fetch(b0, 0)

        for c in wcopies(0, (1, 2)):
            c.start()
        for i in range(1, nc):
            for c in wcopies(i):
                c.start()
        oall[...] = jnp.zeros(oall.shape, BF16)
        for c in gcopies:
            c.wait()

        def weights(b, i, part):
            @pl.when(b == b0)
            def _():
                for c in wcopies(i, part):
                    c.wait()

        @pl.loop(b0, b1)
        def _(b):
            slot = lax.rem(b - b0, 2)

            @pl.when(b + 1 < b1)
            def _():
                fetch(b + 1, 1 - slot)

            g = jnp.concatenate(
                [jnp.where(tl_ref[b * BT + j] >= 0,
                           gall[pl.ds(pl.multiple_of(jnp.maximum(tl_ref[b * BT + j] - first * tps, 0) * tile, tile), tile)],
                           jnp.zeros((tile, d), BF16)) for j in range(BT)], axis=0)
            arrive(b, slot)

            @pl.when(b > b0)
            def _():
                for c in half_copies(b - 1):
                    c.wait()

            def col(i):
                c = lax.rem(c0 + i, nc)
                return c, pl.ds(pl.multiple_of(c * fc, fc), fc)

            weights(b, 0, (0,))
            da = _dot_nt(g, w2v[col(0)[1], :])
            for i in range(nc):
                c, cs = col(i)
                weights(b, i, (1, 2))
                if i + 1 < nc:
                    weights(b, i + 1, (0,))
                nxt = _dot_nt(g, w2v[col(i + 1)[1], :]) if i + 1 < nc else None
                a, dh1, dh3 = _grads(da, h1b[slot, :, cs], h3b[slot, :, cs])
                if i < nc // 2:
                    hs = pl.ds(i * fc, fc)
                    hb[0, :, hs] = a
                    hb[1, :, hs] = dh1
                    hb[2, :, hs] = dh3
                y = _dot_nt(jnp.concatenate([dh1, dh3], axis=1), w13v[c])
                if i == 0:
                    acc[...] = y
                else:
                    acc[...] += y
                da = nxt
                if i == nc // 2 - 1:
                    for cp in half_copies(b):
                        cp.start()
            for j in range(BT):
                @pl.when(tl_ref[b * BT + j] >= 0)
                def _():
                    t = tl_ref[b * BT + j] - first * tps
                    oall[pl.ds(pl.multiple_of(t * tile, tile), tile)] = acc[pl.ds(j * tile, tile)].astype(BF16)

        @pl.when(b0 >= b1)
        def _():
            for i in range(nc):
                for c in wcopies(i):
                    c.wait()

        outs = [pltpu.make_async_copy(oall.at[pl.ds(q * cap, cap)], dxd_refs[q], osem.at[q]) for q in range(ng)]
        for c in outs:
            c.start()

        @pl.when(b0 < b1)
        def _():
            for c in half_copies(b1 - 1):
                c.wait()

        if alias:
            @pl.when(lax.rem(b1, 2) == 1)
            def _():
                hb[...] = jnp.zeros(hb.shape, BF16)
                for c in half_copies(b1):
                    c.start()
                for c in half_copies(b1):
                    c.wait()
        for c in outs:
            c.wait()

    hshape = jax.ShapeDtypeStruct((nblk * rows, fh), BF16)
    base = 3 + ng + 5
    return pl.pallas_call(
        kernel, in_specs=[SMEM] * 3 + [HBM] * (ng + 5 + (3 if alias else 0)), out_specs=[HBM] * (ng + 3),
        out_shape=[jax.ShapeDtypeStruct((cap, d), BF16)] * ng + [hshape] * 3,
        input_output_aliases={base + q: ng + q for q in range(3)} if alias else {},
        scratch_shapes=[pltpu.VMEM((nc, d, 2 * fc), BF16), pltpu.VMEM((f, d), BF16),
                        pltpu.VMEM((ng * cap, d), BF16), pltpu.VMEM((2, rows, f), BF16), pltpu.VMEM((2, rows, f), BF16),
                        pltpu.VMEM((ng * cap, d), BF16), pltpu.VMEM((3, rows, fh), BF16),
                        pltpu.VMEM((rows, d), F32),
                        pltpu.SemaphoreType.DMA((nc, 3)), pltpu.SemaphoreType.DMA((ng,)),
                        pltpu.SemaphoreType.DMA((2, 2, BT)), pltpu.SemaphoreType.DMA((ng,)),
                        pltpu.SemaphoreType.DMA((3,))],
        compiler_params=_params(), name="own_rows",
        cost_estimate=_cost(2 * 200 * ng * d * f * 3, 5e7),
    )(rng, tl, meta, *gs, h1, h3, w1, w3, w2, *(halves if alias else ()))


def _plan(occ, meta, cut, tps, size):
    nt = occ.shape[0]

    def kernel(occ_ref, meta_ref, tl_ref, bnd_ref):
        me = meta_ref[1]
        pos = jnp.int32(0)
        bnd_ref[0] = pos
        for part, (lo, hi) in enumerate(((0, cut * tps), (cut * tps, nt))):
            def step(t, pos):
                tl_ref[pos] = t
                return pos + occ_ref[lax.bitwise_xor(t // tps, me) * tps + lax.rem(t, tps)]

            pos = lax.fori_loop(lo, hi, step, pos)
            end = ((pos + BT - 1) // BT) * BT

            def pad(i, c):
                tl_ref[i] = -1
                return c

            lax.fori_loop(pos, end if part == 0 else end + BT, pad, 0)
            pos = end
            bnd_ref[1 + part] = pos // BT
        bnd_ref[3] = (pos // BT + 1) // 2

    return pl.pallas_call(
        kernel, in_specs=[SMEM] * 2, out_specs=[SMEM] * 2,
        out_shape=[jax.ShapeDtypeStruct((size,), I32), jax.ShapeDtypeStruct((8,), I32)],
        name="plan", cost_estimate=_cost(1e6, 1e3))(occ, meta)


def _dw(rng, tl, meta, first, gs, x, own, peer, sums, at, bt):
    ng = len(gs)
    cap, d = gs[0].shape
    _, tile, _ = x.shape
    tps = cap // tile
    fh = own[0].shape[1] if own else peer[0].shape[1] // 2
    rows = bt * tile
    fc = FC
    nc = fh // fc
    nadd = 3 if sums else 0
    mb = -(-ng * tps // bt) + (1 if own else 0)

    def kernel(rng_ref, tl_ref, meta_ref, *refs):
        g_refs, x_ref, refs = refs[:ng], refs[ng], refs[ng + 1:]
        s_refs, q_refs, o_refs = refs[:3], refs[3:3 + nadd], refs[3 + nadd:6 + nadd]
        (gall, xb, xt, gb, sv, p1, p3, p2, gsem, xsem, ssem, psem, osem) = refs[6 + nadd:]
        b0, b1 = rng_ref[at[0]], rng_ref[at[1]]
        half, me = meta_ref[0], meta_ref[1]

        def xcopy(b, j):
            t = tl_ref[b * bt + j]
            t = lax.bitwise_xor(t // tps, me) * tps + lax.rem(t, tps)
            return pltpu.make_async_copy(x_ref.at[t], xb.at[b - b0, pl.ds(j * tile, tile)], xsem.at[b - b0, j])

        gcopies = [pltpu.make_async_copy(g_refs[q], gall.at[pl.ds(q * cap, cap)], gsem.at[q]) for q in range(ng)]

        def pcopies(c, slot):
            cs = pl.ds(pl.multiple_of(c * fc, fc), fc)
            views = ((p1, (slice(None), cs)), (p3, (slice(None), cs)), (p2, (cs, slice(None))))
            return [pltpu.make_async_copy(q.at[ix], p.at[slot], psem.at[slot, r])
                    for r, (q, (p, ix)) in enumerate(zip(q_refs, views))]

        def ocopies(c, slot):
            cs = pl.ds(pl.multiple_of(c * fc, fc), fc)
            views = ((p1, (slice(None), cs)), (p3, (slice(None), cs)), (p2, (cs, slice(None))))
            return [pltpu.make_async_copy(p.at[slot], o.at[ix], osem.at[slot, r])
                    for r, (o, (p, ix)) in enumerate(zip(o_refs, views))]

        def wcopies(c, slot):
            cs = pl.ds(pl.multiple_of(half * fh + c * fc, fc), fc)
            return [pltpu.make_async_copy(s.at[:, cs] if r < 2 else s.at[cs], sv.at[slot, r], ssem.at[slot, r])
                    for r, s in enumerate(s_refs)]

        def scopies(c, b, slot):
            rs = pl.ds(pl.multiple_of(b * rows, rows), rows)
            cs = pl.ds(pl.multiple_of(c * fc, fc), fc)
            return [pltpu.make_async_copy(s.at[rs, cs], sv.at[slot, r], ssem.at[slot, r]) for r, s in enumerate(s_refs)]

        for c in gcopies:
            c.start()

        @pl.loop(b0, b1)
        def _(b):
            for j in range(bt):
                @pl.when(tl_ref[b * bt + j] >= 0)
                def _():
                    xcopy(b, j).start()

                @pl.when(tl_ref[b * bt + j] < 0)
                def _():
                    xb[b - b0, pl.ds(j * tile, tile)] = jnp.zeros((tile, d), BF16)

        if peer:
            for cp in wcopies(0, 0):
                cp.start()
        if sums:
            for cp in pcopies(0, 0):
                cp.start()
        if own:
            @pl.when(b0 < b1)
            def _():
                for cp in scopies(0, b0, 0):
                    cp.start()
        for c in gcopies:
            c.wait()

        @pl.loop(b0, b1)
        def _(b):
            for j in range(bt):
                @pl.when(tl_ref[b * bt + j] >= 0)
                def _():
                    xcopy(b, j).wait()
                    t = tl_ref[b * bt + j] - first * tps
                    gb[b - b0, pl.ds(j * tile, tile)] = gall[pl.ds(pl.multiple_of(t * tile, tile), tile)]

                @pl.when(tl_ref[b * bt + j] < 0)
                def _():
                    gb[b - b0, pl.ds(j * tile, tile)] = jnp.zeros((tile, d), BF16)
            xt[b - b0] = xb[b - b0].T

        @pl.loop(0, nc)
        def _(c):
            ps = lax.rem(c, 2)
            if peer:
                @pl.when(c + 1 < nc)
                def _():
                    for cp in wcopies(c + 1, 1 - ps):
                        cp.start()

                for cp in wcopies(c, ps):
                    cp.wait()

            if sums:
                @pl.when(c + 1 < nc)
                def _():
                    @pl.when(c >= 1)
                    def _():
                        for cp in ocopies(c - 1, 1 - ps):
                            cp.wait()

                    for cp in pcopies(c + 1, 1 - ps):
                        cp.start()

                for cp in pcopies(c, ps):
                    cp.wait()
            else:
                @pl.when(c >= 2)
                def _():
                    for cp in ocopies(c - 2, ps):
                        cp.wait()

                p1[ps] = jnp.zeros((d, fc), F32)
                p3[ps] = jnp.zeros((d, fc), F32)
                p2[ps] = jnp.zeros((fc, d), F32)

            @pl.loop(b0, b1)
            def _(b):
                i = b - b0
                if own:
                    slot = lax.rem(c * (b1 - b0) + i, 2)

                    @pl.when(b + 1 < b1)
                    def _():
                        for cp in scopies(c, b + 1, 1 - slot):
                            cp.start()

                    @pl.when((b + 1 == b1) & (c + 1 < nc))
                    def _():
                        for cp in scopies(c + 1, b0, 1 - slot):
                            cp.start()

                    for cp in scopies(c, b, slot):
                        cp.wait()
                    a, dh1, dh3 = sv[slot, 0], sv[slot, 1], sv[slot, 2]
                else:
                    h1 = _dot(xb[i], sv[ps, 0]).astype(BF16)
                    h3 = _dot(xb[i], sv[ps, 1]).astype(BF16)
                    da = _dot_nt(gb[i], sv[ps, 2])
                    a, dh1, dh3 = _grads(da, h1, h3)
                p1[ps] += _dot(xt[i], dh1)
                p3[ps] += _dot(xt[i], dh3)
                p2[ps] += _dot(a.T, gb[i])

            for cp in ocopies(c, ps):
                cp.start()

        for c in (nc - 2, nc - 1):
            for cp in ocopies(c, c % 2):
                cp.wait()

    srows = rows if own else d
    outs = [jax.ShapeDtypeStruct((d, fh), F32), jax.ShapeDtypeStruct((d, fh), F32), jax.ShapeDtypeStruct((fh, d), F32)]
    return pl.pallas_call(
        kernel, in_specs=[SMEM] * 3 + [HBM] * (ng + 4 + nadd), out_specs=[HBM] * 3, out_shape=outs,
        scratch_shapes=[pltpu.VMEM((ng * cap, d), BF16), pltpu.VMEM((mb, rows, d), BF16), pltpu.VMEM((mb, d, rows), BF16),
                        pltpu.VMEM((mb, rows, d), BF16), pltpu.VMEM((2, 3, srows, fc), BF16),
                        pltpu.VMEM((2, d, fc), F32), pltpu.VMEM((2, d, fc), F32), pltpu.VMEM((2, fc, d), F32),
                        pltpu.SemaphoreType.DMA((ng,)), pltpu.SemaphoreType.DMA((mb, bt)),
                        pltpu.SemaphoreType.DMA((2, 3)), pltpu.SemaphoreType.DMA((2, 3)), pltpu.SemaphoreType.DMA((2, 3))],
        compiler_params=_params(), name="own_dw" if own else "peer_dw",
        cost_estimate=_cost(2 * 200 * ng * d * fh * (3 if own else 6), 5e7),
    )(rng, tl, meta, *gs, x, *(own or peer), *(sums or ()))


def solution(mesh):
    ne = mesh.shape['expert']
    nd = mesh.shape['data']
    tok = P(('data', 'expert'), None)
    buf = P(('data', 'expert'), None, None)
    wsp = P('expert', None, None)
    zswap = [(i, nd - 1 - i) for i in range(nd)]
    ka = ne * 3 // 4
    groups = ((2, 4, 3, 5), (6, 7, 1, 0))

    def run(dy, gates, topk_idx, slot, yd, xd, h1, h3, w1, w3, w2):
        t, d = dy.shape
        cap = xd.shape[1] // ne
        f = w1.shape[2]
        nt = xd.shape[1] // TILE
        tps = cap // TILE
        me = lax.axis_index('expert').astype(I32)
        grp = lax.axis_index('data').astype(I32)
        meta = jnp.stack([grp, me])
        xor = lambda k: [(i, i ^ k) for i in range(ne)]
        swap = lambda v: lax.ppermute(v, 'data', zswap)

        x4 = xd.reshape(nt, TILE, d)
        xo = swap(x4)

        send = [None] * ne
        for ks in groups:
            for k, v in zip(ks, _scatter_rows(topk_idx.reshape(1, t), slot.reshape(1, t), gates.reshape(1, t), dy, meta, ks, cap)):
                send[k] = v
        dyd = [send[0]]
        for k in range(1, ne):
            dyd.append(lax.ppermute(send[k], 'expert', xor(k)))
        dyo = []
        for k in range(ne):
            dyo.append(swap(dyd[k]))

        occ = jnp.any(x4 != 0, axis=(1, 2)).astype(I32)
        occo = swap(occ)
        nblk = -(-ka * tps // BT) + -(-(ne - ka) * tps // BT) + 1
        tl, bnd = _plan(occ, meta, ka, tps, (nblk + 1) * BT)
        tlo, bndo = _plan(occo, meta, ka, tps, (nblk + 1) * BT)

        h14, h34 = h1.reshape(nt, TILE, f), h3.reshape(nt, TILE, f)
        wts = (w1[0], w3[0], w2[0])
        *da, ha, hd1, hd3 = _own_rows(bnd, tl, meta, 0, dyd[:ka], h14, h34, *wts, None, nblk, (0, 1))
        back = [da[0]]
        for k in range(1, ka):
            back.append(lax.ppermute(da[k], 'expert', xor(k)))
        *db, ha, hd1, hd3 = _own_rows(bnd, tl, meta, ka, dyd[ka:], h14, h34, *wts, (ha, hd1, hd3), nblk, (1, 2))
        for k in range(ka, ne):
            back.append(lax.ppermute(db[k - ka], 'expert', xor(k)))
        sums = _dw(bnd, tl, meta, 0, dyd, x4, (ha, hd1, hd3), None, None, (0, 3), 2 * BT)
        dg = jnp.einsum('tkd,td->tk', yd, dy, preferred_element_type=F32)
        cpos = jnp.where(slot >= 0, (topk_idx ^ me) * cap + slot, -1)
        dx = _gather_rows(cpos, back)
        sums = _dw(bndo, tlo, meta, 0, dyo[:ka], xo, None, wts, sums, (0, 1), BT)
        sums = _dw(bndo, tlo, meta, ka, dyo[ka:], xo, None, wts, sums, (1, 2), BT)
        dw1, dw3, dw2 = sums
        return dx, dg, dw1[None], dw3[None], dw2[None]


    return jax.shard_map(run, mesh=mesh,
                         in_specs=(tok, tok, tok, tok, buf, buf, buf, buf, wsp, wsp, wsp),
                         out_specs=(tok, tok, P('expert', None, 'data'), P('expert', None, 'data'), P('expert', 'data', None)),
                         check_vma=False)
```

```python
import jax
import jax.numpy as jnp
from jax import lax
from jax.experimental import pallas as pl
from jax.experimental.pallas import tpu as pltpu
from jax.sharding import PartitionSpec as P


F32 = jnp.float32
BF16 = jnp.bfloat16
I32 = jnp.int32


TILE = 64
BT = 4
FC = 768
VMEM_LIMIT = 62 * 1024 * 1024

ANY = pl.BlockSpec(memory_space=pl.ANY)
HBM = pl.BlockSpec(memory_space=pltpu.HBM)
SMEM = pl.BlockSpec(memory_space=pltpu.SMEM)


def _params(**kw):
    return pltpu.CompilerParams(vmem_limit_bytes=VMEM_LIMIT, **kw)


def _cost(flops, nbytes):
    return pl.CostEstimate(flops=int(flops), bytes_accessed=int(nbytes), transcendentals=0)


def _dot(a, b):
    return jnp.dot(a, b, preferred_element_type=F32)


def _dot_nt(a, b):
    return lax.dot_general(a, b, (((1,), (1,)), ((), ())), preferred_element_type=F32)


def _grads(da, h1, h3):
    h1f = h1.astype(F32)
    h3f = h3.astype(F32)
    da = da.astype(BF16).astype(F32)
    s = jax.nn.sigmoid(h1f)
    silu = h1f * s
    a = (silu * h3f).astype(BF16)
    dh1 = ((da * h3f) * (s + silu * (1.0 - s))).astype(BF16)
    dh3 = (da * silu).astype(BF16)
    return a, dh1, dh3


def _scatter_rows(topk, slot, gates, dy, me, ks, cap):
    t, d = dy.shape
    k = len(ks)

    def kernel(meta_ref, e_ref, s_ref, g_ref, dy_ref, *refs):
        outs, v_ref, ob, sem = refs[:k], refs[k], refs[k + 1], refs[k + 2]
        col = jnp.broadcast_to(g_ref[...], (128, t)).T
        for c in range(0, d, 128):
            v_ref[:, c:c + 128] = (col * dy_ref[:, c:c + 128].astype(F32)).astype(BF16)

        @pl.loop(0, k)
        def _(q):
            kq = sum(jnp.where(q == p, ks[p], 0) for p in range(k))
            pos = jnp.where(e_ref[...] == lax.bitwise_xor(kq, meta_ref[1]), s_ref[...], -1)
            row = lax.broadcasted_iota(I32, (cap, t), 0)
            oh = jnp.where(pos == row, 1.0, 0.0).astype(BF16)
            ob[q] = _dot(oh, v_ref[...]).astype(BF16)
            for p in range(k):
                @pl.when(q == p)
                def _():
                    pltpu.make_async_copy(ob.at[p], outs[p], sem.at[p]).start()

        for p in range(k):
            pltpu.make_async_copy(ob.at[p], outs[p], sem.at[p]).wait()

    vm = pl.BlockSpec(memory_space=pltpu.VMEM)
    return pl.pallas_call(
        kernel, in_specs=[SMEM] + [vm] * 4, out_specs=[HBM] * k,
        out_shape=[jax.ShapeDtypeStruct((cap, d), BF16)] * k,
        scratch_shapes=[pltpu.VMEM((t, d), BF16), pltpu.VMEM((k, cap, d), BF16), pltpu.SemaphoreType.DMA((k,))],
        compiler_params=_params(), name="scatter_rows",
        cost_estimate=_cost(2 * k * cap * t * d, 2 * k * cap * d * 2),
    )(me, topk, slot, gates, dy)


def _gather_rows(pos, parts):
    t = pos.shape[0]
    k = len(parts)
    r, d = parts[0].shape
    tb = 512

    def kernel(pos_ref, *refs):
        ins, o_ref, src, sem = refs[:k], refs[k], refs[k + 1], refs[k + 2]

        @pl.when(pl.program_id(0) == 0)
        def _():
            for q in range(k):
                pltpu.make_async_copy(ins[q], src.at[pl.ds(q * r, r)], sem.at[q]).start()
            for q in range(k):
                pltpu.make_async_copy(ins[q], src.at[pl.ds(q * r, r)], sem.at[q]).wait()

        col = lax.broadcasted_iota(I32, (tb, k * r), 1)
        oh = jnp.where(pos_ref[...] == col, 1.0, 0.0).astype(BF16)
        o_ref[...] = _dot(oh, src[...]).astype(BF16)

    return pl.pallas_call(
        kernel, grid=(t // tb,),
        in_specs=[pl.BlockSpec((tb, 1), lambda i: (i, 0))] + [HBM] * k,
        out_specs=pl.BlockSpec((tb, d), lambda i: (i, 0)),
        out_shape=jax.ShapeDtypeStruct((t, d), BF16),
        scratch_shapes=[pltpu.VMEM((k * r, d), BF16), pltpu.SemaphoreType.DMA((k,))],
        compiler_params=_params(), name="gather_rows",
        cost_estimate=_cost(2 * k * r * t * d, 2 * k * r * d * 2),
    )(pos, *parts)


def _own_rows(rng, tl, meta, first, gs, h1, h3, w1, w3, w2, halves, nblk, at):
    ng = len(gs)
    cap, d = gs[0].shape
    _, tile, f = h1.shape
    tps = cap // tile
    fh = f // 2
    rows = BT * tile
    fc = 512
    nc = f // fc
    alias = halves is not None

    def kernel(rng_ref, tl_ref, meta_ref, *refs):
        g_refs, refs = refs[:ng], refs[ng:]
        h1_ref, h3_ref, w1_hbm, w3_hbm, w2_hbm = refs[:5]
        refs = refs[5 + (3 if alias else 0):]
        dxd_refs, gcat_ref, refs = refs[:ng], refs[ng], refs[ng + 1:]
        (a_ref, dh1_ref, dh3_ref, w13v, w2v, gall, h1b, h3b, oall, hb, acc,
         wsem, gsem, isem, osem, hsem, csem) = refs
        b0, b1 = rng_ref[at[0]], rng_ref[at[1]]
        half, me = meta_ref[0], meta_ref[1]
        c0 = half * (nc // 2)

        def src_tile(t):
            return lax.bitwise_xor(t // tps, me) * tps + lax.rem(t, tps)

        def tile_copies(b, slot, j):
            t = src_tile(tl_ref[b * BT + j])
            rs = pl.ds(j * tile, tile)
            return (pltpu.make_async_copy(h1_ref.at[t], h1b.at[slot, rs], isem.at[slot, 0, j]),
                    pltpu.make_async_copy(h3_ref.at[t], h3b.at[slot, rs], isem.at[slot, 1, j]))

        def fetch(b, slot):
            for j in range(BT):
                @pl.when(tl_ref[b * BT + j] >= 0)
                def _():
                    for c in tile_copies(b, slot, j):
                        c.start()

                @pl.when(tl_ref[b * BT + j] < 0)
                def _():
                    rs = pl.ds(j * tile, tile)
                    h1b[slot, rs] = jnp.zeros((tile, f), BF16)
                    h3b[slot, rs] = jnp.zeros((tile, f), BF16)

        def arrive(b, slot):
            for j in range(BT):
                @pl.when(tl_ref[b * BT + j] >= 0)
                def _():
                    for c in tile_copies(b, slot, j):
                        c.wait()

        def half_copies(b):
            rs = pl.ds(pl.multiple_of(b * rows, rows), rows)
            return [pltpu.make_async_copy(hb.at[q], r.at[rs], hsem.at[q])
                    for q, r in enumerate((a_ref, dh1_ref, dh3_ref))]

        gcopies = [pltpu.make_async_copy(g_refs[q], gall.at[pl.ds(q * cap, cap)], gsem.at[q]) for q in range(ng)]

        def wcopies(i, parts=(0, 1, 2)):
            c = lax.rem(c0 + i, nc)
            cs = pl.ds(pl.multiple_of(c * fc, fc), fc)
            return [pltpu.make_async_copy(w2_hbm.at[cs], w2v.at[cs], wsem.at[i, 0]) if q == 0 else
                    pltpu.make_async_copy((w1_hbm, w3_hbm)[q - 1].at[:, cs], w13v.at[c, :, pl.ds((q - 1) * fc, fc)],
                                          wsem.at[i, q])
                    for q in parts]

        for c in gcopies + wcopies(0, (0,)):
            c.start()

        @pl.when(b0 < b1)
        def _():
            fetch(b0, 0)

        for c in wcopies(0, (1, 2)):
            c.start()
        for i in range(1, nc):
            for c in wcopies(i):
                c.start()
        oall[...] = jnp.zeros(oall.shape, BF16)
        for c in gcopies:
            c.wait()
        gcat = pltpu.make_async_copy(gall, gcat_ref, csem.at[0])
        gcat.start()

        def weights(b, i, part):
            @pl.when(b == b0)
            def _():
                for c in wcopies(i, part):
                    c.wait()

        @pl.loop(b0, b1)
        def _(b):
            slot = lax.rem(b - b0, 2)

            @pl.when(b + 1 < b1)
            def _():
                fetch(b + 1, 1 - slot)

            g = jnp.concatenate(
                [jnp.where(tl_ref[b * BT + j] >= 0,
                           gall[pl.ds(pl.multiple_of(jnp.maximum(tl_ref[b * BT + j] - first * tps, 0) * tile, tile), tile)],
                           jnp.zeros((tile, d), BF16)) for j in range(BT)], axis=0)
            arrive(b, slot)

            @pl.when(b > b0)
            def _():
                for c in half_copies(b - 1):
                    c.wait()

            def col(i):
                c = lax.rem(c0 + i, nc)
                return c, pl.ds(pl.multiple_of(c * fc, fc), fc)

            weights(b, 0, (0,))
            da = _dot_nt(g, w2v[col(0)[1], :])
            for i in range(nc):
                c, cs = col(i)
                weights(b, i, (1, 2))
                if i + 1 < nc:
                    weights(b, i + 1, (0,))
                nxt = _dot_nt(g, w2v[col(i + 1)[1], :]) if i + 1 < nc else None
                a, dh1, dh3 = _grads(da, h1b[slot, :, cs], h3b[slot, :, cs])
                if i < nc // 2:
                    hs = pl.ds(i * fc, fc)
                    hb[0, :, hs] = a
                    hb[1, :, hs] = dh1
                    hb[2, :, hs] = dh3
                y = _dot_nt(jnp.concatenate([dh1, dh3], axis=1), w13v[c])
                if i == 0:
                    acc[...] = y
                else:
                    acc[...] += y
                da = nxt
                if i == nc // 2 - 1:
                    for cp in half_copies(b):
                        cp.start()
            for j in range(BT):
                @pl.when(tl_ref[b * BT + j] >= 0)
                def _():
                    t = tl_ref[b * BT + j] - first * tps
                    oall[pl.ds(pl.multiple_of(t * tile, tile), tile)] = acc[pl.ds(j * tile, tile)].astype(BF16)

        @pl.when(b0 >= b1)
        def _():
            for i in range(nc):
                for c in wcopies(i):
                    c.wait()

        outs = [pltpu.make_async_copy(oall.at[pl.ds(q * cap, cap)], dxd_refs[q], osem.at[q]) for q in range(ng)]
        for c in outs:
            c.start()

        @pl.when(b0 < b1)
        def _():
            for c in half_copies(b1 - 1):
                c.wait()

        if alias:
            @pl.when(lax.rem(b1, 2) == 1)
            def _():
                hb[...] = jnp.zeros(hb.shape, BF16)
                for c in half_copies(b1):
                    c.start()
                for c in half_copies(b1):
                    c.wait()
        gcat.wait()
        for c in outs:
            c.wait()

    hshape = jax.ShapeDtypeStruct((nblk * rows, fh), BF16)
    base = 3 + ng + 5
    return pl.pallas_call(
        kernel, in_specs=[SMEM] * 3 + [HBM] * (ng + 5 + (3 if alias else 0)), out_specs=[HBM] * (ng + 4),
        out_shape=[jax.ShapeDtypeStruct((cap, d), BF16)] * ng + [jax.ShapeDtypeStruct((ng * cap, d), BF16)] + [hshape] * 3,
        input_output_aliases={base + q: ng + 1 + q for q in range(3)} if alias else {},
        scratch_shapes=[pltpu.VMEM((nc, d, 2 * fc), BF16), pltpu.VMEM((f, d), BF16),
                        pltpu.VMEM((ng * cap, d), BF16), pltpu.VMEM((2, rows, f), BF16), pltpu.VMEM((2, rows, f), BF16),
                        pltpu.VMEM((ng * cap, d), BF16), pltpu.VMEM((3, rows, fh), BF16),
                        pltpu.VMEM((rows, d), F32),
                        pltpu.SemaphoreType.DMA((nc, 3)), pltpu.SemaphoreType.DMA((ng,)),
                        pltpu.SemaphoreType.DMA((2, 2, BT)), pltpu.SemaphoreType.DMA((ng,)),
                        pltpu.SemaphoreType.DMA((3,)), pltpu.SemaphoreType.DMA((1,))],
        compiler_params=_params(), name="own_rows",
        cost_estimate=_cost(2 * 200 * ng * d * f * 3, 5e7),
    )(rng, tl, meta, *gs, h1, h3, w1, w3, w2, *(halves if alias else ()))


def _plan(occ, meta, cut, tps, size):
    nt = occ.shape[0]

    def kernel(occ_ref, meta_ref, tl_ref, bnd_ref):
        me = meta_ref[1]
        pos = jnp.int32(0)
        bnd_ref[0] = pos
        for part, (lo, hi) in enumerate(((0, cut * tps), (cut * tps, nt))):
            def step(t, pos):
                tl_ref[pos] = t
                return pos + occ_ref[lax.bitwise_xor(t // tps, me) * tps + lax.rem(t, tps)]

            pos = lax.fori_loop(lo, hi, step, pos)
            end = ((pos + BT - 1) // BT) * BT

            def pad(i, c):
                tl_ref[i] = -1
                return c

            lax.fori_loop(pos, end if part == 0 else end + BT, pad, 0)
            pos = end
            bnd_ref[1 + part] = pos // BT
        bnd_ref[3] = (pos // BT + 1) // 2

    return pl.pallas_call(
        kernel, in_specs=[SMEM] * 2, out_specs=[SMEM] * 2,
        out_shape=[jax.ShapeDtypeStruct((size,), I32), jax.ShapeDtypeStruct((8,), I32)],
        name="plan", cost_estimate=_cost(1e6, 1e3))(occ, meta)


def _dw(rng, tl, meta, first, gs, x, own, peer, sums, at, bt, tps):
    ng = len(gs)
    _, tile, d = x.shape
    offs = [sum(g.shape[0] for g in gs[:q]) for q in range(ng + 1)]
    gtiles = offs[ng] // tile
    fh = own[0].shape[1] if own else peer[0].shape[1] // 2
    rows = bt * tile
    fc = FC
    nc = fh // fc
    nadd = 3 if sums else 0
    mb = -(-gtiles // bt) + (1 if own else 0)

    def kernel(rng_ref, tl_ref, meta_ref, *refs):
        g_refs, x_ref, refs = refs[:ng], refs[ng], refs[ng + 1:]
        s_refs, q_refs, o_refs = refs[:3], refs[3:3 + nadd], refs[3 + nadd:6 + nadd]
        (gall, xb, xt, gb, sv, p1, p3, p2, gsem, xsem, ssem, psem, osem) = refs[6 + nadd:]
        b0, b1 = rng_ref[at[0]], rng_ref[at[1]]
        half, me = meta_ref[0], meta_ref[1]

        def xcopy(b, j):
            t = tl_ref[b * bt + j]
            t = lax.bitwise_xor(t // tps, me) * tps + lax.rem(t, tps)
            return pltpu.make_async_copy(x_ref.at[t], xb.at[b - b0, pl.ds(j * tile, tile)], xsem.at[b - b0, j])

        gcopies = [pltpu.make_async_copy(g_refs[q], gall.at[pl.ds(offs[q], offs[q + 1] - offs[q])], gsem.at[q])
                   for q in range(ng)]

        def pcopies(c, slot):
            cs = pl.ds(pl.multiple_of(c * fc, fc), fc)
            views = ((p1, (slice(None), cs)), (p3, (slice(None), cs)), (p2, (cs, slice(None))))
            return [pltpu.make_async_copy(q.at[ix], p.at[slot], psem.at[slot, r])
                    for r, (q, (p, ix)) in enumerate(zip(q_refs, views))]

        def ocopies(c, slot):
            cs = pl.ds(pl.multiple_of(c * fc, fc), fc)
            views = ((p1, (slice(None), cs)), (p3, (slice(None), cs)), (p2, (cs, slice(None))))
            return [pltpu.make_async_copy(p.at[slot], o.at[ix], osem.at[slot, r])
                    for r, (o, (p, ix)) in enumerate(zip(o_refs, views))]

        def wcopies(c, slot):
            cs = pl.ds(pl.multiple_of(half * fh + c * fc, fc), fc)
            return [pltpu.make_async_copy(s.at[:, cs] if r < 2 else s.at[cs], sv.at[slot, r], ssem.at[slot, r])
                    for r, s in enumerate(s_refs)]

        def scopies(c, b, slot):
            rs = pl.ds(pl.multiple_of(b * rows, rows), rows)
            cs = pl.ds(pl.multiple_of(c * fc, fc), fc)
            return [pltpu.make_async_copy(s.at[rs, cs], sv.at[slot, r], ssem.at[slot, r]) for r, s in enumerate(s_refs)]

        for c in gcopies:
            c.start()

        @pl.loop(b0, b1)
        def _(b):
            for j in range(bt):
                @pl.when(tl_ref[b * bt + j] >= 0)
                def _():
                    xcopy(b, j).start()

                @pl.when(tl_ref[b * bt + j] < 0)
                def _():
                    xb[b - b0, pl.ds(j * tile, tile)] = jnp.zeros((tile, d), BF16)

        if peer:
            for cp in wcopies(0, 0):
                cp.start()
        if sums:
            for cp in pcopies(0, 0):
                cp.start()
        if own:
            @pl.when(b0 < b1)
            def _():
                for cp in scopies(0, b0, 0):
                    cp.start()
        for c in gcopies:
            c.wait()

        def ready(b):
            for j in range(bt):
                @pl.when(tl_ref[b * bt + j] >= 0)
                def _():
                    xcopy(b, j).wait()
                    t = tl_ref[b * bt + j] - first * tps
                    gb[b - b0, pl.ds(j * tile, tile)] = gall[pl.ds(pl.multiple_of(t * tile, tile), tile)]

                @pl.when(tl_ref[b * bt + j] < 0)
                def _():
                    gb[b - b0, pl.ds(j * tile, tile)] = jnp.zeros((tile, d), BF16)
            xt[b - b0] = xb[b - b0].T

        @pl.loop(0, nc)
        def _(c):
            ps = lax.rem(c, 2)
            if peer:
                @pl.when(c + 1 < nc)
                def _():
                    for cp in wcopies(c + 1, 1 - ps):
                        cp.start()

                for cp in wcopies(c, ps):
                    cp.wait()

            if sums:
                @pl.when(c + 1 < nc)
                def _():
                    @pl.when(c >= 1)
                    def _():
                        for cp in ocopies(c - 1, 1 - ps):
                            cp.wait()

                    for cp in pcopies(c + 1, 1 - ps):
                        cp.start()

                for cp in pcopies(c, ps):
                    cp.wait()
            else:
                @pl.when(c >= 2)
                def _():
                    for cp in ocopies(c - 2, ps):
                        cp.wait()

                @pl.when(b0 >= b1)
                def _():
                    for p in (p1, p3, p2):
                        p[ps] = jnp.zeros(p.shape[1:], F32)

            @pl.loop(b0, b1)
            def _(b):
                i = b - b0

                @pl.when(c == 0)
                def _():
                    ready(b)

                if own:
                    slot = lax.rem(c * (b1 - b0) + i, 2)

                    @pl.when(b + 1 < b1)
                    def _():
                        for cp in scopies(c, b + 1, 1 - slot):
                            cp.start()

                    @pl.when((b + 1 == b1) & (c + 1 < nc))
                    def _():
                        for cp in scopies(c + 1, b0, 1 - slot):
                            cp.start()

                    for cp in scopies(c, b, slot):
                        cp.wait()
                    a, dh1, dh3 = sv[slot, 0], sv[slot, 1], sv[slot, 2]
                else:
                    h1 = _dot(xb[i], sv[ps, 0]).astype(BF16)
                    h3 = _dot(xb[i], sv[ps, 1]).astype(BF16)
                    da = _dot_nt(gb[i], sv[ps, 2])
                    a, dh1, dh3 = _grads(da, h1, h3)
                base = (lambda p: p[ps]) if sums else (lambda p: jnp.where(i > 0, p[ps], 0.0))
                p1[ps] = base(p1) + _dot(xt[i], dh1)
                p3[ps] = base(p3) + _dot(xt[i], dh3)
                p2[ps] = base(p2) + _dot(a.T, gb[i])

            for cp in ocopies(c, ps):
                cp.start()

        for c in (nc - 2, nc - 1):
            for cp in ocopies(c, c % 2):
                cp.wait()

    srows = rows if own else d
    outs = [jax.ShapeDtypeStruct((d, fh), F32), jax.ShapeDtypeStruct((d, fh), F32), jax.ShapeDtypeStruct((fh, d), F32)]
    return pl.pallas_call(
        kernel, in_specs=[SMEM] * 3 + [HBM] * (ng + 4 + nadd), out_specs=[HBM] * 3, out_shape=outs,
        scratch_shapes=[pltpu.VMEM((offs[ng], d), BF16), pltpu.VMEM((mb, rows, d), BF16), pltpu.VMEM((mb, d, rows), BF16),
                        pltpu.VMEM((mb, rows, d), BF16), pltpu.VMEM((2, 3, srows, fc), BF16),
                        pltpu.VMEM((2, d, fc), F32), pltpu.VMEM((2, d, fc), F32), pltpu.VMEM((2, fc, d), F32),
                        pltpu.SemaphoreType.DMA((ng,)), pltpu.SemaphoreType.DMA((mb, bt)),
                        pltpu.SemaphoreType.DMA((2, 3)), pltpu.SemaphoreType.DMA((2, 3)), pltpu.SemaphoreType.DMA((2, 3))],
        compiler_params=_params(), name="own_dw" if own else "peer_dw",
        cost_estimate=_cost(2 * 40 * gtiles * d * fh * (3 if own else 6), 5e7),
    )(rng, tl, meta, *gs, x, *(own or peer), *(sums or ()))


def solution(mesh):
    ne = mesh.shape['expert']
    nd = mesh.shape['data']
    tok = P(('data', 'expert'), None)
    buf = P(('data', 'expert'), None, None)
    wsp = P('expert', None, None)
    zswap = [(i, nd - 1 - i) for i in range(nd)]
    ka = ne * 3 // 4
    groups = ((2, 4, 3, 5), (6, 7, 1, 0))

    def run(dy, gates, topk_idx, slot, yd, xd, h1, h3, w1, w3, w2):
        t, d = dy.shape
        cap = xd.shape[1] // ne
        f = w1.shape[2]
        nt = xd.shape[1] // TILE
        tps = cap // TILE
        me = lax.axis_index('expert').astype(I32)
        grp = lax.axis_index('data').astype(I32)
        meta = jnp.stack([grp, me])
        xor = lambda k: [(i, i ^ k) for i in range(ne)]
        swap = lambda v: lax.ppermute(v, 'data', zswap)

        x4 = xd.reshape(nt, TILE, d)
        xo = swap(x4)

        send = [None] * ne
        for ks in groups:
            for k, v in zip(ks, _scatter_rows(topk_idx.reshape(1, t), slot.reshape(1, t), gates.reshape(1, t), dy, meta, ks, cap)):
                send[k] = v
        dyd = [send[0]]
        for k in range(1, ne):
            dyd.append(lax.ppermute(send[k], 'expert', xor(k)))
        occ = jnp.any(x4 != 0, axis=(1, 2)).astype(I32)
        occo = swap(occ)
        nblk = -(-ka * tps // BT) + -(-(ne - ka) * tps // BT) + 1
        tl, bnd = _plan(occ, meta, ka, tps, (nblk + 1) * BT)
        tlo, bndo = _plan(occo, meta, ka, tps, (nblk + 1) * BT)

        h14, h34 = h1.reshape(nt, TILE, f), h3.reshape(nt, TILE, f)
        wts = (w1[0], w3[0], w2[0])
        *da, ga, ha, hd1, hd3 = _own_rows(bnd, tl, meta, 0, dyd[:ka], h14, h34, *wts, None, nblk, (0, 1))
        goa = swap(ga)
        back = [da[0]]
        for k in range(1, ka):
            back.append(lax.ppermute(da[k], 'expert', xor(k)))
        *db, gb, ha, hd1, hd3 = _own_rows(bnd, tl, meta, ka, dyd[ka:], h14, h34, *wts, (ha, hd1, hd3), nblk, (1, 2))
        gob = swap(gb)
        for k in range(ka, ne):
            back.append(lax.ppermute(db[k - ka], 'expert', xor(k)))
        sums = _dw(bnd, tl, meta, 0, [ga, gb], x4, (ha, hd1, hd3), None, None, (0, 3), 2 * BT, tps)
        dg = jnp.einsum('tkd,td->tk', yd, dy, preferred_element_type=F32)
        cpos = jnp.where(slot >= 0, (topk_idx ^ me) * cap + slot, -1)
        dx = _gather_rows(cpos, back)
        sums = _dw(bndo, tlo, meta, 0, [goa], xo, None, wts, sums, (0, 1), BT, tps)
        sums = _dw(bndo, tlo, meta, ka, [gob], xo, None, wts, sums, (1, 2), BT, tps)
        dw1, dw3, dw2 = sums
        return dx, dg, dw1[None], dw3[None], dw2[None]


    return jax.shard_map(run, mesh=mesh,
                         in_specs=(tok, tok, tok, tok, buf, buf, buf, buf, wsp, wsp, wsp),
                         out_specs=(tok, tok, P('expert', None, 'data'), P('expert', None, 'data'), P('expert', 'data', None)),
                         check_vma=False)
```
